256 devices in a mesh: grp: 4 (over y_hi, core), blk: 64 (over z, x, y_lo).
Axes of the slice: x: 4, y: 4 (y_hi: 2, y_lo: 2; y = y_hi * 2 + y_lo), z: 8, core: 2. Of those that a mesh axis runs over, the one named last changes fastest.
Arguments:
- primal: float32 [2097152], P(('blk', 'grp')), may hold values from -3 to 3
- dual: float32 [1048576], P(('blk', 'grp')), may hold values from -3 to 3
- objective: float32 [2097152], P(('blk', 'grp')), may hold values from -6 to 6
- lower: float32 [2097152], P(('blk', 'grp')), may hold values from -2 to -0.5
- upper: float32 [2097152], P(('blk', 'grp')), may hold values from 0.5 to 2
- bound_kind: int32 [2097152], P(('blk', 'grp')), may hold values from 0 to 3
- rhs: float32 [1048576], P(('blk', 'grp')), may hold values from -6 to 6
- row_kind: int32 [1048576], P(('blk', 'grp')), may hold values 0 or 1
- q_tiles: float32 [4, 256, 512, 512], P('grp', 'blk'), may hold values from -0.25 to 0.25
- q_index: int32 [4, 2, 256], P('grp', None, 'blk'), may hold values from 0 to 1023
- k_tiles: float32 [4, 384, 512, 512], P('grp', 'blk'), may hold values from -0.25 to 0.25
- k_rows: int32 [4, 384], P('grp', 'blk'), may hold values from 0 to 31
- k_cols: int32 [4, 384], P('grp', 'blk'), may hold values from 0 to 1023
Outputs:
- final_primal: float32 [2097152], P(('blk', 'grp'))
- final_dual: float32 [1048576], P(('blk', 'grp'))
- primal_weight: float32 [], replicated
The draws below stay inside these ranges and needn't reach their ends.
Inputs may be any that keep to these rules, and one draw needn't show every extreme that they name: `q_index`: row and column tile indices of Hessian tiles, within the column group. `k_rows`: row tile within the tile's dual block. `bound_kind`: 0 free, 1 lower bound only, 2 both bounds, 3 upper bound only.
All inputs are finite; a program needn't handle non-finite values. No bound on the sum of `row_kind` on one device may be relied on, other than what follows from the above.
Results may differ from the reference program's by a relative error of at most 0.00017.
Values sent between devices are 32-bit elements; how exact they have to be, the bound alone decides.
A program may use at most 64 MiB of HBM per device.

```python
import jax
import jax.numpy as jnp
from jax import lax

TILE = 512
X_DEV = 8192
Y_DEV = 4096
KT = 6
ITERS = 2
NX = 2097152
M = 1048576
GT_COUNT = 1024
RT = 32
QTILES = 256
KTILES = 384
N_GRP = 4
N_BLK = 64


def place_ends(result, rng, smallest, top_value):
    dims = result.shape
    place = [jax.random.randint(jax.random.fold_in(rng, axis), (), 0, dims[axis]) for axis in range(len(dims))]
    result = result.at[tuple(place)].set(smallest)
    longest = dims.index(max(dims))
    place[longest] = (place[longest] + 1) % dims[longest]
    return result.at[tuple(place)].set(top_value)


def steps_of(key, extent, split, low, largest):
    def one(axis_at, blocks):
        draws = jax.random.uniform(jax.random.fold_in(jax.random.fold_in(key, 6), axis_at), (blocks,), jnp.float32, low / len(split), largest / len(split))
        return jnp.repeat(jnp.exp(draws), extent[axis_at] // blocks).reshape((-1,) + (1,) * (len(extent) - axis_at - 1))

    gain = one(*split[0])
    for cut in split[1:]:
        gain = gain * one(*cut)
    return gain


def scatter_about(key, shape, spread, reach, cuts=(), kind=jnp.bfloat16):
    result = spread * jax.random.normal(key, shape, jnp.float32)
    if cuts:
        result = result * steps_of(key, shape, cuts, -0.22, 0.18)
    return jnp.clip(result, -reach, reach).astype(kind)


def setup_inputs(seed: int = 0) -> dict:
    keys = jax.random.split(jax.random.key(seed), 14)
    return {
        "primal": scatter_about(keys[0], (NX,), 0.5, 3.0, ((0, 256),), jnp.float32),
        "dual": scatter_about(keys[1], (M,), 0.5, 3.0, ((0, 256),), jnp.float32),
        "objective": scatter_about(keys[2], (NX,), 1.0, 6.0, ((0, 256),), jnp.float32),
        "lower": jnp.clip(-2.0 + 1.5 * jax.random.uniform(keys[3], (NX,), jnp.float32) ** steps_of(keys[3], (NX,), ((0, 256),), -0.2, 0.2), -2.0, -0.5),
        "upper": jnp.clip(0.5 + 1.5 * jax.random.uniform(keys[4], (NX,), jnp.float32) ** steps_of(keys[4], (NX,), ((0, 256),), -0.2, 0.2), 0.5, 2.0),
        "bound_kind": place_ends(jax.random.randint(keys[5], (NX,), 0, 4), jax.random.fold_in(keys[5], 1), 0, 3).astype(jnp.int32),
        "rhs": scatter_about(keys[6], (M,), 1.0, 6.0, ((0, 256),), jnp.float32),
        "row_kind": place_ends((jax.random.randint(keys[7], (M,), 0, 2) < 1).astype(jnp.int32), jax.random.fold_in(keys[7], 1), 0, 1),
        "q_tiles": scatter_about(keys[8], (N_GRP, QTILES, TILE, TILE), TILE ** -0.5, 0.25, ((0, 4), (1, 64)), jnp.float32),
        "q_index": place_ends(jax.random.randint(keys[9], (N_GRP, 2, QTILES), 0, GT_COUNT), jax.random.fold_in(keys[9], 1), 0, GT_COUNT - 1).astype(jnp.int32),
        "k_tiles": scatter_about(keys[10], (N_GRP, KTILES, TILE, TILE), TILE ** -0.5, 0.25, ((0, 4), (1, 64)), jnp.float32),
        "k_rows": place_ends(jax.random.randint(keys[11], (N_GRP, KTILES), 0, RT), jax.random.fold_in(keys[11], 1), 0, RT - 1).astype(jnp.int32),
        "k_cols": place_ends(jax.random.randint(keys[12], (N_GRP, KTILES), 0, GT_COUNT), jax.random.fold_in(keys[12], 1), 0, GT_COUNT - 1).astype(jnp.int32),
    }


def apply_tiles(tiles, rows, cols, vec, count):
    pieces = vec.reshape(-1, TILE)[cols]
    product = jnp.einsum('tij,tj->ti', tiles, pieces, precision=lax.Precision.HIGHEST)
    return jnp.zeros((count, TILE), product.dtype).at[rows].add(product).reshape(-1)

def apply_transposed(tiles, rows, cols, vec, count):
    pieces = vec.reshape(-1, TILE)[rows]
    product = jnp.einsum('tij,ti->tj', tiles, pieces, precision=lax.Precision.HIGHEST)
    return jnp.zeros((count, TILE), product.dtype).at[cols].add(product).reshape(-1)

def project(values, lower, upper, bound_kind):
    values = jnp.where((bound_kind == 1) | (bound_kind == 2), jnp.maximum(values, lower), values)
    return jnp.where((bound_kind == 2) | (bound_kind == 3), jnp.minimum(values, upper), values)

def reference(primal, dual, objective, lower, upper, bound_kind, rhs, row_kind, q_tiles, q_index, k_tiles, k_rows, k_cols):
    group_tiles = N_BLK * X_DEV // TILE
    block_tiles = N_GRP * Y_DEV // TILE
    owner = (jnp.arange(N_BLK * KT) // KT).astype(jnp.int32)

    def group_vec(values, group):
        return values.reshape(N_BLK, N_GRP, X_DEV)[:, group, :].reshape(-1)

    def to_layout(parts):
        return jnp.stack([p.reshape(N_BLK, X_DEV) for p in parts], axis=1).reshape(-1)

    def forward(values):
        cons_prod = None
        parts = []
        for group in range(N_GRP):
            column_vec = group_vec(values, group)
            parts.append(apply_tiles(q_tiles[group], q_index[group, 0], q_index[group, 1], column_vec, group_tiles))
            term = apply_tiles(k_tiles[group], owner * block_tiles + k_rows[group], k_cols[group], column_vec, N_BLK * block_tiles)
            cons_prod = term if cons_prod is None else cons_prod + term
        return (cons_prod, to_layout(parts))

    def transposed(duals):
        parts = []
        for group in range(N_GRP):
            parts.append(apply_transposed(k_tiles[group], owner * block_tiles + k_rows[group], k_cols[group], duals, group_tiles))
        return to_layout(parts)
    weight = jnp.asarray(1.0, jnp.float32)
    current, duals = (primal, dual)
    cons_prod, hess_prod = forward(current)
    for step in range(ITERS):
        step_primal = 0.5 / weight
        step_dual = 0.5 * weight
        gradient = hess_prod + objective - transposed(duals)
        updated = project(current - step_primal * gradient, lower, upper, bound_kind)
        next_cons, next_hess = forward(updated)
        extrap = 2.0 * next_cons - cons_prod
        dual_new = duals + step_dual * (rhs - extrap)
        dual_new = jnp.where(row_kind == 1, jnp.maximum(dual_new, 0.0), dual_new)
        primal_sq = jnp.sum((updated - current) ** 2)
        dual_sq = jnp.sum((dual_new - duals) ** 2)
        weight = jnp.sqrt(weight * jnp.sqrt((dual_sq + 1e-06) / (primal_sq + 1e-06)))
        current, duals = (updated, dual_new)
        cons_prod, hess_prod = (next_cons, next_hess)
    return (current, duals, weight)
```

```python
import jax
import jax.numpy as jnp
from jax import lax
from jax.experimental import pallas as pl
from jax.experimental.pallas import tpu as pltpu
from jax.sharding import Mesh
from jax.sharding import PartitionSpec as P

F32 = jnp.float32
BF16 = jnp.bfloat16
MESH = pl.DeviceIdType.MESH
EPSILON = 1e-06
STEP_SCALE = 0.5
FAR = 1e30


def split3(v):
    hi = v.astype(BF16)
    rest = v - hi.astype(F32)
    mid = rest.astype(BF16)
    low = (rest - mid.astype(F32)).astype(BF16)
    return hi, mid, low


def pick(onehot, data):
    parts = [jnp.dot(onehot, part, preferred_element_type=F32) for part in split3(data)]
    return parts[0] + (parts[1] + parts[2])


def onehot(cond):
    return jnp.where(cond, 1.0, 0.0).astype(BF16)


def iota(shape, dim):
    return lax.broadcasted_iota(jnp.int32, shape, dim)


def folded(v):
    return jnp.sum(v.reshape(-1, 8, 128), axis=0)


def scalar_sum(v):
    return jnp.sum(jnp.sum(v, axis=0, keepdims=True), axis=1, keepdims=True)


def kernel(
    x_h, y_h, c_h, lo_h, hi_h, bk_h, b_h, rk_h, q_h, k_h, qi_s, kr_s, kc_s,
    xo_h, yo_h, w_s,
    tiles, bounds, kinds, rkind,
    xpl, cpl, ydat, idz, idp, idg, nidz, tid, sel, ed, ysel, e,
    sx, xr, sc, cr, xs, cst, yrows, ys, kp, zprod, sp, gp, dbuf, wz, wp,
    loc, tsem, zs, zr, ps, pr, gs, gr,
):
    z = lax.axis_index("z")
    px, py = lax.axis_index("x"), lax.axis_index("yl")
    gh, gl = lax.axis_index("yh"), lax.axis_index("co")
    p, g = px * 2 + py, gh * 2 + gl
    pending = []

    loads = {}
    for n, (name, src, dst) in enumerate((
        ("x", x_h, xpl.at[p]),
        ("y", y_h, ydat.at[g, 0]),
        ("b", b_h, ydat.at[g, 1]),
        ("rk", rk_h, rkind),
        ("c", c_h, cpl.at[p, 0]),
        ("lo", lo_h, bounds.at[0]),
        ("hi", hi_h, bounds.at[1]),
        ("bk", bk_h, kinds),
    )):
        loads[name] = pltpu.make_async_copy(src, dst, loc.at[n])
        loads[name].start()
    tile_loads = []
    for t in range(10):
        src = q_h.at[0, t] if t < 4 else k_h.at[0, t - 4]
        tile_loads.append(pltpu.make_async_copy(src, tiles.at[t], tsem.at[t]))
        tile_loads[-1].start()

    def z_peer(k):
        return {"z": lax.rem(z + k, 8)}

    def p_peer(k):
        return {"x": lax.rem(px + k // 2, 4), "yl": lax.rem(py + k % 2, 2)}

    def g_peer(k):
        return {"yh": lax.rem(gh + k // 2, 2), "co": lax.rem(gl + k % 2, 2)}

    def send(count, peer, ssem, rsem, stage, source, target):
        copies = []
        for k in range(1, count):
            copies.append(pltpu.make_async_remote_copy(
                src_ref=source(k), dst_ref=target, send_sem=ssem.at[stage, k - 1], recv_sem=rsem.at[stage, k - 1],
                device_id=peer(k), device_id_type=MESH,
            ))
            copies[-1].start()
        pending.extend(copies)
        return copies

    def send_z(stage, source, target):
        return send(8, z_peer, zs, zr, stage, source, target)

    def send_p(stage, source, target):
        return send(8, p_peer, ps, pr, stage, source, target)

    def send_g(stage, source, target):
        return send(4, g_peer, gs, gr, stage, source, target)

    def arrive(copies):
        for copy in copies:
            copy.wait_recv()

    lane, sub = iota((8, 128), 1), iota((8, 128), 0)

    def ids_at(place, ids):
        slot = place // 4
        value = jnp.zeros((8, 128), jnp.int32)
        for n, scalar in enumerate(ids):
            value = jnp.where(slot == n, scalar, value)
        return jnp.where((place >= 0) & (place < 4 * len(ids)), value * 4 + place % 4 + 1, 0)

    cons_cols = [kc_s[0, t] for t in range(6)]
    sent = [qi_s[0, 0, t] for t in range(4)] + cons_cols
    need = [qi_s[0, 1, t] for t in range(4)] + cons_cols
    rows = [kr_s[0, t] for t in range(6)]
    sent_v = ids_at(sub * 128 + lane - z * 64, sent)
    need_v = ids_at(lane, need)
    rows_v = ids_at(lane - g * 32, rows)
    ids = jnp.where(sub < 4, sent_v, jnp.where(sub == 4, need_v, jnp.where(sub == 5, rows_v, 0))).astype(F32)
    idz[z] = ids
    idp[p] = ids
    idg[g] = ids
    for zz in range(8):
        zprod[0, zz, 40:64, :] = jnp.zeros((24, 128), F32)
        zprod[1, zz, 40:64, :] = jnp.zeros((24, 128), F32)

    barrier = pltpu.get_barrier_semaphore()
    for k in range(1, 8):
        pl.semaphore_signal(barrier, inc=1, device_id=z_peer(k), device_id_type=MESH)
        pl.semaphore_signal(barrier, inc=1, device_id=p_peer(k), device_id_type=MESH)
    for k in range(1, 4):
        pl.semaphore_signal(barrier, inc=1, device_id=g_peer(k), device_id_type=MESH)
    pl.semaphore_wait(barrier, 17)

    loads["x"].wait()
    x_plane = send_p(0, lambda k: xpl.at[p], xpl.at[p])
    id_z = send_z(0, lambda k: idz.at[z], idz.at[z])
    id_p = send_p(1, lambda k: idp.at[p], idp.at[p])
    id_g = send_g(0, lambda k: idg.at[g], idg.at[g])
    loads["y"].wait()
    loads["b"].wait()
    loads["rk"].wait()
    ydat[g, 2] = rkind[...].astype(F32)
    y_all = send_g(1, lambda k: ydat.at[g], ydat.at[g])
    loads["c"].wait()
    loads["lo"].wait()
    loads["hi"].wait()
    loads["bk"].wait()
    kind = kinds[...]
    cpl[p, 1] = jnp.where((kind == 1) | (kind == 2), bounds[0], -FAR)
    cpl[p, 2] = jnp.where((kind == 2) | (kind == 3), bounds[1], FAR)
    c_plane = send_p(2, lambda k: cpl.at[p], cpl.at[p])

    arrive(id_z)
    eye40 = iota((40, 128), 0) == iota((40, 128), 1)

    def column(row, mask):
        return jnp.sum(jnp.where(mask, row, 0.0), axis=1, keepdims=True)

    for zz in range(8):
        nidz[40 * zz : 40 * zz + 40, :] = jnp.broadcast_to(column(idz[zz, 4:5, :], eye40), (40, 128))
    for n in range(4):
        have = (z * 512 + n * 128 + 1 + iota((1, 128), 1)).astype(F32)
        sel[:, n * 128 : (n + 1) * 128] = onehot(nidz[...] == have)

    arrive(x_plane)
    sx[...] = pick(sel[...], xpl[...].reshape(512, 128)).reshape(8, 40, 128)
    xr[z] = sx[z]
    x_slots = send_z(1, lambda k: sx.at[lax.rem(z + k, 8)], xr.at[z])
    xs[0, 0:64, :] = xpl[p]

    arrive(id_g)
    eye32 = iota((32, 128), 1) == iota((32, 128), 0) + g * 32
    own_rows = column(idg[g, 5:6, :], eye32)
    ysel[...] = onehot(own_rows == (iota((32, 128), 1) + 1).astype(F32))
    all_rows = idg[0, 5:6, :] + idg[1, 5:6, :] + idg[2, 5:6, :] + idg[3, 5:6, :]
    ed[...] = onehot((iota((128, 128), 0) + 1).astype(F32) == all_rows)
    arrive(id_p)
    for pp in range(8):
        own = ((z * 8 + pp) * 64 + 1 + iota((64, 128), 0)).astype(F32)
        tid[104 * pp : 104 * pp + 64, :] = own
        tid[104 * pp + 64 : 104 * pp + 104, :] = jnp.broadcast_to(column(idp[pp, 4:5, :], eye40), (40, 128))
    made = idz[0, 0:4, :]
    for zz in range(1, 8):
        made = made + idz[zz, 0:4, :]
    for n in range(4):
        e[:, n * 128 : (n + 1) * 128] = onehot(tid[...] == made[n : n + 1, :])

    eye = iota((128, 128), 0) == iota((128, 128), 1)

    def forward(first, pairs, source, store):
        def body(i, _):
            x8 = source(i)
            out = jnp.zeros((8, 128), F32)
            for h in range(2):
                for r in range(4):
                    total = None
                    for n in range(4):
                        part = tiles[first + 2 * i + h, r * 128 : (r + 1) * 128, n * 128 : (n + 1) * 128]
                        part = part * x8[4 * h + n : 4 * h + n + 1, :]
                        total = part if total is None else total + part
                    col = jnp.sum(total, axis=1, keepdims=True)
                    row = jnp.sum(jnp.where(eye, col, 0.0), axis=0, keepdims=True)
                    out = jnp.where(sub == 4 * h + r, row, out)
            store(i, out)
            return 0

        lax.fori_loop(0, pairs, body, 0)

    def transposed(stage):
        def body(i, _):
            y8 = yrows[pl.ds(pl.multiple_of(8 * i, 8), 8), :]
            out = jnp.zeros((8, 128), F32)
            for h in range(2):
                totals = [None] * 4
                for r in range(4):
                    col = column(y8[4 * h + r : 4 * h + r + 1, :], eye)
                    for n in range(4):
                        part = tiles[4 + 2 * i + h, r * 128 : (r + 1) * 128, n * 128 : (n + 1) * 128]
                        part = folded(part * col)
                        totals[n] = part if totals[n] is None else totals[n] + part
                for n in range(4):
                    row = jnp.sum(totals[n], axis=0, keepdims=True)
                    out = jnp.where(sub == 4 * h + n, row, out)
            zprod[stage, z, pl.ds(pl.multiple_of(16 + 8 * i, 8), 8), :] = -out
            return 0

        lax.fori_loop(0, 3, body, 0)

    def hess(step):
        def source(i):
            return xs[step, pl.ds(pl.multiple_of(64 + 8 * i, 8), 8), :]

        def store(i, out):
            zprod[step, z, pl.ds(pl.multiple_of(8 * i, 8), 8), :] = out

        forward(0, 2, source, store)

    def cons(step):
        def source(i):
            return xs[step, pl.ds(pl.multiple_of(80 + 8 * i, 8), 8), :]

        def store(i, out):
            kp[step, pl.ds(pl.multiple_of(8 * i, 8), 8), :] = out

        forward(4, 3, source, store)

    arrive(y_all)
    ys[0] = ydat[:, 0].reshape(128, 128)
    for copy in tile_loads:
        copy.wait()
    yrows[...] = pick(ysel[...], ys[0])
    transposed(0)

    arrive(x_slots)
    xs[0, 64:104, :] = jnp.sum(xr[...], axis=0)
    hess(0)
    prod_z = send_z(2, lambda k: zprod.at[0, z, pl.ds(0, 40)], zprod.at[0, z, pl.ds(0, 40)])

    arrive(c_plane)
    for a in range(3):
        sc[:, a] = pick(sel[...], cpl[:, a].reshape(512, 128)).reshape(8, 40, 128)
        cr[z, a] = sc[z, a]
    c_slots = send_z(3, lambda k: sc.at[lax.rem(z + k, 8)], cr.at[z])
    for a in range(3):
        cst[a, 0:64, :] = cpl[p, a]
    cons(0)

    weight = jnp.ones((1, 1), F32)
    for step in range(2):
        arrive(prod_z)
        sp[step] = pick(e[...], zprod[step].reshape(512, 128)).reshape(8, 104, 128)
        gp[step, p] = sp[step, p]
        grads = []
        for k in range(1, 8):
            to = lax.rem(px + k // 2, 4) * 2 + lax.rem(py + k % 2, 2)
            grads.append(to)
        grad_p = send_p(3 + step, lambda k: sp.at[step, grads[k - 1]], gp.at[step, p])
        if step == 0:
            arrive(c_slots)
            for a in range(3):
                cst[a, 64:104, :] = jnp.sum(cr[:, a], axis=0)
        else:
            arrive(w_p)
            sums = jnp.sum(wp[step - 1], axis=0)
            weight = jnp.sqrt(weight * jnp.sqrt((scalar_sum(sums[8:16]) + EPSILON) / (scalar_sum(sums[0:8]) + EPSILON)))
        step_primal = STEP_SCALE / weight
        step_dual = STEP_SCALE * weight
        arrive(grad_p)
        gradient = jnp.sum(gp[step], axis=0) + cst[0]
        current = xs[step]
        updated = jnp.minimum(jnp.maximum(current - step_primal * gradient, cst[1]), cst[2])
        xs[step + 1] = updated
        moved = updated[0:64] - current[0:64]
        if step == 1:
            x_out = pltpu.make_async_copy(xs.at[2, pl.ds(0, 64)], xo_h, loc.at[8])
            x_out.start()

        cons(step + 1)
        dbuf[step, g, 0:24, :] = 2.0 * kp[step + 1] - kp[step]
        dbuf[step, g, 24:32, :] = folded(moved * moved)
        duals_g = send_g(2 + step, lambda k: dbuf.at[step, g], dbuf.at[step, g])
        if step == 0:
            hess(1)
        arrive(duals_g)
        extrap = pick(ed[...], dbuf[step].reshape(128, 128))
        duals = ys[step]
        dual_new = duals + step_dual * (ydat[:, 1].reshape(128, 128) - extrap)
        dual_new = jnp.where(ydat[:, 2].reshape(128, 128) == 1.0, jnp.maximum(dual_new, 0.0), dual_new)
        ys[step + 1] = dual_new
        moved = dual_new - duals
        wz[step, z, 0:8, :] = jnp.sum(dbuf[step, :, 24:32, :], axis=0)
        wz[step, z, 8:16, :] = folded(moved * moved)
        if step == 0:
            yrows[...] = pick(ysel[...], dual_new)
            transposed(1)
            prod_z = send_z(4, lambda k: zprod.at[1, z, pl.ds(0, 40)], zprod.at[1, z, pl.ds(0, 40)])
        else:
            y_out = pltpu.make_async_copy(ys.at[2, pl.ds(pl.multiple_of(g * 32, 32), 32)], yo_h, loc.at[9])
            y_out.start()
        w_z = send_z(5 + step, lambda k: wz.at[step, z], wz.at[step, z])
        arrive(w_z)
        wp[step, p] = jnp.sum(wz[step], axis=0)
        w_p = send_p(5 + step, lambda k: wp.at[step, p], wp.at[step, p])

    arrive(w_p)
    sums = jnp.sum(wp[1], axis=0)
    weight = jnp.sqrt(weight * jnp.sqrt((scalar_sum(sums[8:16]) + EPSILON) / (scalar_sum(sums[0:8]) + EPSILON)))
    w_s[0, 0] = weight[0, 0]
    x_out.wait()
    y_out.wait()
    for copy in pending:
        copy.wait_send()


def shards(primal, dual, objective, lower, upper, bound_kind, rhs, row_kind, q_tiles, q_index, k_tiles, k_rows, k_cols):
    hbm = pl.BlockSpec(memory_space=pl.ANY)
    smem = pl.BlockSpec(memory_space=pltpu.SMEM)
    vmem, dma = pltpu.VMEM, pltpu.SemaphoreType.DMA

    def lines(v):
        return v.reshape(-1, 128)

    final_x, final_y, weight = pl.pallas_call(
        kernel,
        name="pdhg",
        out_shape=(
            jax.ShapeDtypeStruct((64, 128), F32),
            jax.ShapeDtypeStruct((32, 128), F32),
            jax.ShapeDtypeStruct((1, 1), F32),
        ),
        in_specs=[hbm] * 10 + [smem] * 3,
        out_specs=(hbm, hbm, smem),
        scratch_shapes=[
            vmem((10, 512, 512), F32),
            vmem((2, 64, 128), F32),
            vmem((64, 128), jnp.int32),
            vmem((32, 128), jnp.int32),
            vmem((8, 64, 128), F32),
            vmem((8, 3, 64, 128), F32),
            vmem((4, 3, 32, 128), F32),
            vmem((8, 8, 128), F32),
            vmem((8, 8, 128), F32),
            vmem((4, 8, 128), F32),
            vmem((320, 128), F32),
            vmem((832, 128), F32),
            vmem((320, 512), BF16),
            vmem((128, 128), BF16),
            vmem((32, 128), BF16),
            vmem((832, 512), BF16),
            vmem((8, 40, 128), F32),
            vmem((8, 40, 128), F32),
            vmem((8, 3, 40, 128), F32),
            vmem((8, 3, 40, 128), F32),
            vmem((3, 104, 128), F32),
            vmem((3, 104, 128), F32),
            vmem((32, 128), F32),
            vmem((3, 128, 128), F32),
            vmem((3, 24, 128), F32),
            vmem((2, 8, 64, 128), F32),
            vmem((2, 8, 104, 128), F32),
            vmem((2, 8, 104, 128), F32),
            vmem((2, 4, 32, 128), F32),
            vmem((2, 8, 16, 128), F32),
            vmem((2, 8, 16, 128), F32),
            dma((10,)),
            dma((10,)),
            dma((7, 7)),
            dma((7, 7)),
            dma((7, 7)),
            dma((7, 7)),
            dma((4, 3)),
            dma((4, 3)),
        ],
        compiler_params=pltpu.CompilerParams(
            collective_id=0, has_side_effects=True, vmem_limit_bytes=48 * 1024 * 1024
        ),
    )(
        lines(primal), lines(dual), lines(objective), lines(lower), lines(upper), lines(bound_kind),
        lines(rhs), lines(row_kind), q_tiles, k_tiles, q_index, k_rows, k_cols,
    )
    return final_x.reshape(-1), final_y.reshape(-1), weight.reshape(())


def solution(mesh):
    finer = Mesh(mesh.devices.reshape(2, 2, 8, 4, 2), ("yh", "co", "z", "x", "yl"))
    grp, blk, both = ("yh", "co"), ("z", "x", "yl"), ("z", "x", "yl", "yh", "co")
    placed = (P(both),) * 8 + (
        P(grp, blk, None, None),
        P(grp, None, blk),
        P(grp, blk, None, None),
        P(grp, blk),
        P(grp, blk),
    )
    return jax.shard_map(shards, mesh=finer, in_specs=placed, out_specs=(P(both), P(both), P()), check_vma=False)
```

```python
import jax
import jax.numpy as jnp
from jax import lax
from jax.experimental import pallas as pl
from jax.experimental.pallas import tpu as pltpu
from jax.sharding import Mesh
from jax.sharding import PartitionSpec as P

F32 = jnp.float32
BF16 = jnp.bfloat16
MESH = pl.DeviceIdType.MESH
EPSILON = 1e-06
STEP_SCALE = 0.5
FAR = 1e30


def halves(v):
    hi = v.astype(BF16)
    mid = (v - hi.astype(F32)).astype(BF16)
    return jnp.concatenate([hi, mid], axis=1)


def pick(onehot, pair):
    both = jnp.dot(onehot, pair, preferred_element_type=F32)
    return both[:, 0:128] + both[:, 128:256]


def onehot(cond):
    return jnp.where(cond, 1.0, 0.0).astype(BF16)


def iota(shape, dim):
    return lax.broadcasted_iota(jnp.int32, shape, dim)


def folded(v):
    return jnp.sum(v.reshape(-1, 8, 128), axis=0)


def scalar_sum(v):
    return jnp.sum(jnp.sum(v, axis=0, keepdims=True), axis=1, keepdims=True)


def kernel(
    x_h, y_h, c_h, lo_h, hi_h, bk_h, b_h, rk_h, q_h, k_h, qi_h, kr_h, kc_h,
    xo_h, yo_h, w_s,
    tiles, bounds, kinds, rkind,
    xpl, cpl, y0, rows, idz, idp, idg, nid, sel, es, eo, ed, ysel,
    sx, xr, sc, cr, xs, cst, yrows, ys, kp, zprod, sps, spo, gps, gpo, dbuf, wz, wp,
    qi_s, kr_s, kc_s, loc, zs, zr, ps, pr, gs, gr, ws, wr,
):
    z = lax.axis_index("z")
    px, py = lax.axis_index("x"), lax.axis_index("yl")
    gh, gl = lax.axis_index("yh"), lax.axis_index("co")
    p, g = px * 2 + py, gh * 2 + gl
    pending = []

    def z_peer(k):
        return {"z": lax.rem(z + k, 8)}

    def p_peer(k):
        return {"x": lax.rem(px + k // 2, 4), "yl": lax.rem(py + k % 2, 2)}

    def g_peer(k):
        return {"yh": lax.rem(gh + k // 2, 2), "co": lax.rem(gl + k % 2, 2)}

    def w_peer(k):
        return {**p_peer(k // 4), **g_peer(k % 4)}

    def p_index(k):
        return lax.rem(px + k // 2, 4) * 2 + lax.rem(py + k % 2, 2)

    barrier = pltpu.get_barrier_semaphore()
    for k in range(1, 8):
        pl.semaphore_signal(barrier, inc=1, device_id=z_peer(k), device_id_type=MESH)
    for k in range(1, 32):
        pl.semaphore_signal(barrier, inc=1, device_id=w_peer(k), device_id_type=MESH)

    def load(n, *pairs):
        for src, dst in pairs:
            pltpu.make_async_copy(src, dst, loc.at[n]).start()

    def loaded(n, part):
        pltpu.make_async_copy(part, part, loc.at[n]).wait()

    index_loads = [
        pltpu.make_async_copy(src, dst, loc.at[n])
        for n, (src, dst) in enumerate(((qi_h, qi_s), (kr_h, kr_s), (kc_h, kc_s)))
    ]
    for copy in index_loads:
        copy.start()
    load(3, (x_h, xpl.at[p]))
    load(4, (y_h, y0.at[g]))
    load(5, (c_h, cpl.at[0, p]), (lo_h, bounds.at[0]), (hi_h, bounds.at[1]), (bk_h, kinds))
    load(6, (b_h, rows.at[g, 0]), (rk_h, rkind))
    load(7, *((k_h.at[0, t], tiles.at[4 + t]) for t in range(6)))
    load(8, *((q_h.at[0, t], tiles.at[t]) for t in range(4)))

    def send(count, peer, ssem, rsem, stage, source, target, whole):
        for k in range(1, count):
            pltpu.make_async_remote_copy(
                src_ref=source(k), dst_ref=target, send_sem=ssem.at[stage], recv_sem=rsem.at[stage],
                device_id=peer(k), device_id_type=MESH,
            ).start()
        pending.append((whole, ssem.at[stage]))
        return whole, rsem.at[stage]

    def send_z(stage, source, target, whole):
        return send(8, z_peer, zs, zr, stage, source, target, whole)

    def send_p(stage, source, target, whole):
        return send(8, p_peer, ps, pr, stage, source, target, whole)

    def send_g(stage, source, target, whole):
        return send(4, g_peer, gs, gr, stage, source, target, whole)

    def send_w(stage, source, target, whole):
        return send(32, w_peer, ws, wr, stage, source, target, whole)

    def arrive(stage):
        whole, sem = stage
        pltpu.make_async_copy(whole, whole, sem).wait()

    lane, sub = iota((4, 128), 1), iota((4, 128), 0)
    sub8 = iota((8, 128), 0)

    def ids_at(place, ids):
        slot = place // 4
        value = jnp.zeros((4, 128), jnp.int32)
        for n, scalar in enumerate(ids):
            value = jnp.where(slot == n, scalar, value)
        return jnp.where((place >= 0) & (place < 4 * len(ids)), value * 4 + place % 4 + 1, 0)

    for copy in index_loads:
        copy.wait()
    cons_cols = [kc_s[0, t] for t in range(6)]
    sent_v = ids_at(lane - lax.rem(z, 2) * 64, [qi_s[0, 0, t] for t in range(4)] + cons_cols)
    need_v = ids_at(lane, [qi_s[0, 1, t] for t in range(4)] + cons_cols)
    rows_v = ids_at(lane - g * 24, [kr_s[0, t] for t in range(6)])
    ids = jnp.where(sub == 0, sent_v, jnp.where(sub == 1, need_v, jnp.where(sub == 2, rows_v, 0))).astype(F32)
    idz[z] = ids
    idp[p] = ids
    idg[g] = ids
    for zz in range(8):
        zprod[0, zz, 40:64, :] = jnp.zeros((24, 128), F32)
        zprod[1, zz, 40:64, :] = jnp.zeros((24, 128), F32)

    pl.semaphore_wait(barrier, 38)

    id_z = send_z(0, lambda k: idz.at[z], idz.at[z], idz.at[pl.ds(0, 7)])
    loaded(3, x_h)
    x_plane = send_p(0, lambda k: xpl.at[p], xpl.at[p], xpl.at[pl.ds(0, 7)])
    loaded(4, y_h)
    y_all = send_g(1, lambda k: y0.at[g], y0.at[g], y0.at[pl.ds(0, 3)])
    id_g = send_g(0, lambda k: idg.at[g], idg.at[g], idg.at[pl.ds(0, 3)])
    id_p = send_p(1, lambda k: idp.at[p], idp.at[p], idp.at[pl.ds(0, 7)])
    loaded(5, cpl.at[0, pl.ds(0, 4)])
    kind = kinds[...]
    cpl[1, p] = jnp.where((kind == 1) | (kind == 2), bounds[0], -FAR)
    cpl[2, p] = jnp.where((kind == 2) | (kind == 3), bounds[1], FAR)
    c_plane = [send_p(2 + a, lambda k: cpl.at[a, p], cpl.at[a, p], cpl.at[a, pl.ds(0, 7)]) for a in range(3)]
    loaded(6, rows.at[0])
    rows[g, 1] = rkind[...].astype(F32)
    rows_all = send_g(2, lambda k: rows.at[g], rows.at[g], rows.at[pl.ds(0, 3)])

    eye40 = iota((40, 128), 0) == iota((40, 128), 1)

    def column(row, mask):
        return jnp.sum(jnp.where(mask, row, 0.0), axis=1, keepdims=True)

    arrive(id_z)
    for zz in range(8):
        nid[40 * zz : 40 * zz + 40, :] = jnp.broadcast_to(column(idz[zz, 1:2, :], eye40), (40, 128))
    for n in range(4):
        have = (z * 512 + n * 128 + 1 + iota((1, 128), 1)).astype(F32)
        sel[:, n * 128 : (n + 1) * 128] = onehot(nid[...] == have)

    arrive(x_plane)
    sx[...] = pick(sel[...], halves(xpl[...].reshape(512, 128))).reshape(8, 40, 128)
    xr[z] = sx[z]
    x_slots = send_z(1, lambda k: sx.at[lax.rem(z + k, 8)], xr.at[z], xr.at[pl.ds(0, 7)])
    xs[0, 0:64, :] = xpl[p]

    eye = iota((128, 128), 0) == iota((128, 128), 1)

    def forward(first, pairs, source, store):
        def body(i, _):
            x8 = source(i)
            out = jnp.zeros((8, 128), F32)
            for h in range(2):
                for r in range(4):
                    total = None
                    for n in range(4):
                        part = tiles[first + 2 * i + h, r * 128 : (r + 1) * 128, n * 128 : (n + 1) * 128]
                        part = part * x8[4 * h + n : 4 * h + n + 1, :]
                        total = part if total is None else total + part
                    col = jnp.sum(total, axis=1, keepdims=True)
                    row = jnp.sum(jnp.where(eye, col, 0.0), axis=0, keepdims=True)
                    out = jnp.where(sub8 == 4 * h + r, row, out)
            store(i, out)
            return 0

        lax.fori_loop(0, pairs, body, 0)

    def transposed(stage):
        def body(i, _):
            y8 = yrows[pl.ds(pl.multiple_of(8 * i, 8), 8), :]
            out = jnp.zeros((8, 128), F32)
            for h in range(2):
                totals = [None] * 4
                for r in range(4):
                    col = column(y8[4 * h + r : 4 * h + r + 1, :], eye)
                    for n in range(4):
                        part = tiles[4 + 2 * i + h, r * 128 : (r + 1) * 128, n * 128 : (n + 1) * 128]
                        part = folded(part * col)
                        totals[n] = part if totals[n] is None else totals[n] + part
                for n in range(4):
                    row = jnp.sum(totals[n], axis=0, keepdims=True)
                    out = jnp.where(sub8 == 4 * h + n, row, out)
            zprod[stage, z, pl.ds(pl.multiple_of(16 + 8 * i, 8), 8), :] = -out
            return 0

        lax.fori_loop(0, 3, body, 0)

    def hess(step):
        def source(i):
            return xs[step, pl.ds(pl.multiple_of(64 + 8 * i, 8), 8), :]

        def store(i, out):
            zprod[step, z, pl.ds(pl.multiple_of(8 * i, 8), 8), :] = out

        forward(0, 2, source, store)

    def cons(step):
        def source(i):
            return xs[step, pl.ds(pl.multiple_of(80 + 8 * i, 8), 8), :]

        def store(i, out):
            kp[step, pl.ds(pl.multiple_of(8 * i, 8), 8), :] = out

        forward(4, 3, source, store)

    def send_hess(step):
        part = zprod.at[step, z, pl.ds(0, 16)]
        return send_z(5 + 2 * step, lambda k: part, part, zprod.at[step, pl.ds(0, 7), pl.ds(0, 16)])

    def send_trans(step):
        part = zprod.at[step, z, pl.ds(16, 24)]
        return send_z(6 + 2 * step, lambda k: part, part, zprod.at[step, pl.ds(0, 7), pl.ds(16, 24)])

    arrive(id_g)
    eye32 = (iota((32, 128), 1) == iota((32, 128), 0) + g * 24) & (iota((32, 128), 0) < 24)
    ysel[...] = onehot(column(idg[g, 2:3, :], eye32) == (iota((32, 128), 1) + 1).astype(F32))
    arrive(y_all)
    ys[0] = y0[...].reshape(128, 128)
    loaded(7, tiles.at[pl.ds(0, 6)])
    yrows[...] = pick(ysel[...], halves(ys[0]))
    transposed(0)
    trans_z = send_trans(0)

    loaded(8, tiles.at[pl.ds(0, 4)])
    arrive(x_slots)
    xs[0, 64:104, :] = jnp.sum(xr[...], axis=0)
    hess(0)
    hess_z = send_hess(0)

    c_slots = []
    for a in range(3):
        arrive(c_plane[a])
        sc[a] = pick(sel[...], halves(cpl[a].reshape(512, 128))).reshape(8, 40, 128)
        cr[a, z] = sc[a, z]
        c_slots.append(
            send_z(2 + a, lambda k: sc.at[a, lax.rem(z + k, 8)], cr.at[a, z], cr.at[a, pl.ds(0, 7)])
        )
        cst[a, 0:64, :] = cpl[a, p]

    arrive(id_p)
    for pp in range(8):
        nid[40 * pp : 40 * pp + 40, :] = jnp.broadcast_to(column(idp[pp, 1:2, :], eye40), (40, 128))
    own = (z * 512 + 1 + iota((512, 128), 0)).astype(F32)
    for n in range(4):
        made = idz[2 * n, 0:1, :] + idz[2 * n + 1, 0:1, :]
        es[:, n * 128 : (n + 1) * 128] = onehot(nid[...] == made)
        eo[:, n * 128 : (n + 1) * 128] = onehot(own == made)
    all_rows = idg[0, 2:3, :] + idg[1, 2:3, :] + idg[2, 2:3, :] + idg[3, 2:3, :]
    ed[...] = onehot((iota((128, 128), 0) + 1).astype(F32) == all_rows)[:, 0:96]

    cons(0)

    def next_weight(stage, weight):
        sums = jnp.sum(wp[stage], axis=0)
        total = jnp.sum(sums, axis=1, keepdims=True) + EPSILON
        return jnp.sqrt(weight * jnp.sqrt(total[1:2] / total[0:1]))

    weight = jnp.ones((1, 1), F32)
    for step in range(2):
        arrive(trans_z)
        arrive(hess_z)
        pair = halves(zprod[step].reshape(512, 128))
        sps[step] = pick(es[...], pair).reshape(8, 40, 128)
        gps[step, p] = sps[step, p]
        first = 16 * step
        grad_s = send_p(
            5 + 2 * step,
            lambda k: sps.at[step, p_index(k), pl.ds(first, 40 - first)],
            gps.at[step, p, pl.ds(first, 40 - first)],
            gps.at[step, pl.ds(0, 7), pl.ds(first, 40 - first)],
        )
        spo[step] = pick(eo[...], pair).reshape(8, 64, 128)
        gpo[step, p] = spo[step, p]
        grad_o = send_p(6 + 2 * step, lambda k: spo.at[step, p_index(k)], gpo.at[step, p], gpo.at[step, pl.ds(0, 7)])
        if step == 0:
            for a in range(3):
                arrive(c_slots[a])
                cst[a, 64:104, :] = jnp.sum(cr[a], axis=0)
        else:
            arrive(w_p)
            weight = next_weight(0, weight)
        step_primal = STEP_SCALE / weight
        step_dual = STEP_SCALE * weight

        def advance(a, b, total):
            here = pl.ds(a, b - a)
            current = xs[step, here, :]
            moved = current - step_primal * (total + cst[0, here, :])
            updated = jnp.minimum(jnp.maximum(moved, cst[1, here, :]), cst[2, here, :])
            xs[step + 1, here, :] = updated
            return updated - current

        arrive(grad_s)
        advance(64 + first, 104, jnp.sum(gps[step, :, first:40, :], axis=0))

        cons(step + 1)
        dbuf[step, g] = 2.0 * kp[step + 1] - kp[step]
        duals_g = send_g(3 + step, lambda k: dbuf.at[step, g], dbuf.at[step, g], dbuf.at[step, pl.ds(0, 3)])
        if step == 0:
            hess(1)
            hess_z = send_hess(1)
            arrive(rows_all)
        arrive(grad_o)
        moved = advance(0, 64, jnp.sum(gpo[step], axis=0))
        wz[step, z, 0:1, :] = jnp.sum(moved * moved, axis=0, keepdims=True)
        if step == 1:
            x_out = pltpu.make_async_copy(xs.at[2, pl.ds(0, 64)], xo_h, loc.at[9])
            x_out.start()
        arrive(duals_g)
        extrap = pick(ed[...], halves(dbuf[step].reshape(96, 128)))
        duals = ys[step]
        dual_new = duals + step_dual * (rows[:, 0].reshape(128, 128) - extrap)
        dual_new = jnp.where(rows[:, 1].reshape(128, 128) == 1.0, jnp.maximum(dual_new, 0.0), dual_new)
        ys[step + 1] = dual_new
        moved = dual_new - duals
        wz[step, z, 1:2, :] = jnp.sum(moved * moved, axis=0, keepdims=True) * 0.25
        w_z = send_z(9 + step, lambda k: wz.at[step, z], wz.at[step, z], wz.at[step, pl.ds(0, 7)])
        if step == 0:
            yrows[...] = pick(ysel[...], halves(dual_new))
            transposed(1)
            trans_z = send_trans(1)
        if step == 1:
            y_out = pltpu.make_async_copy(ys.at[2, pl.ds(pl.multiple_of(g * 32, 32), 32)], yo_h, loc.at[10])
            y_out.start()
        arrive(w_z)
        wp[step, p * 4 + g] = jnp.sum(wz[step], axis=0)
        w_p = send_w(step, lambda k: wp.at[step, p * 4 + g], wp.at[step, p * 4 + g], wp.at[step, pl.ds(0, 31)])

    arrive(w_p)
    w_s[0, 0] = next_weight(1, weight)[0, 0]
    x_out.wait()
    y_out.wait()
    for stage in pending:
        arrive(stage)


def shards(primal, dual, objective, lower, upper, bound_kind, rhs, row_kind, q_tiles, q_index, k_tiles, k_rows, k_cols):
    hbm = pl.BlockSpec(memory_space=pl.ANY)
    smem = pl.BlockSpec(memory_space=pltpu.SMEM)
    vmem, dma = pltpu.VMEM, pltpu.SemaphoreType.DMA

    def lines(v):
        return v.reshape(-1, 128)

    final_x, final_y, weight = pl.pallas_call(
        kernel,
        name="pdhg",
        out_shape=(
            jax.ShapeDtypeStruct((64, 128), F32),
            jax.ShapeDtypeStruct((32, 128), F32),
            jax.ShapeDtypeStruct((1, 1), F32),
        ),
        in_specs=[hbm] * 13,
        out_specs=(hbm, hbm, smem),
        scratch_shapes=[
            vmem((10, 512, 512), F32),
            vmem((2, 64, 128), F32),
            vmem((64, 128), jnp.int32),
            vmem((32, 128), jnp.int32),
            vmem((8, 64, 128), F32),
            vmem((3, 8, 64, 128), F32),
            vmem((4, 32, 128), F32),
            vmem((4, 2, 32, 128), F32),
            vmem((8, 4, 128), F32),
            vmem((8, 4, 128), F32),
            vmem((4, 4, 128), F32),
            vmem((320, 128), F32),
            vmem((320, 512), BF16),
            vmem((320, 512), BF16),
            vmem((512, 512), BF16),
            vmem((128, 96), BF16),
            vmem((32, 128), BF16),
            vmem((8, 40, 128), F32),
            vmem((8, 40, 128), F32),
            vmem((3, 8, 40, 128), F32),
            vmem((3, 8, 40, 128), F32),
            vmem((3, 104, 128), F32),
            vmem((3, 104, 128), F32),
            vmem((32, 128), F32),
            vmem((3, 128, 128), F32),
            vmem((3, 24, 128), F32),
            vmem((2, 8, 64, 128), F32),
            vmem((2, 8, 40, 128), F32),
            vmem((2, 8, 64, 128), F32),
            vmem((2, 8, 40, 128), F32),
            vmem((2, 8, 64, 128), F32),
            vmem((2, 4, 24, 128), F32),
            vmem((2, 8, 2, 128), F32),
            vmem((2, 32, 2, 128), F32),
            pltpu.SMEM((1, 2, 4), jnp.int32),
            pltpu.SMEM((1, 6), jnp.int32),
            pltpu.SMEM((1, 6), jnp.int32),
            dma((11,)),
            dma((11,)),
            dma((11,)),
            dma((9,)),
            dma((9,)),
            dma((5,)),
            dma((5,)),
            dma((2,)),
            dma((2,)),
        ],
        compiler_params=pltpu.CompilerParams(
            collective_id=0, has_side_effects=True, vmem_limit_bytes=67043328
        ),
    )(
        lines(primal), lines(dual), lines(objective), lines(lower), lines(upper), lines(bound_kind),
        lines(rhs), lines(row_kind), q_tiles, k_tiles, q_index, k_rows, k_cols,
    )
    return final_x.reshape(-1), final_y.reshape(-1), weight.reshape(())


def solution(mesh):
    finer = Mesh(mesh.devices.reshape(2, 2, 8, 4, 2), ("yh", "co", "z", "x", "yl"))
    grp, blk, both = ("yh", "co"), ("z", "x", "yl"), ("z", "x", "yl", "yh", "co")
    placed = (P(both),) * 8 + (
        P(grp, blk, None, None),
        P(grp, None, blk),
        P(grp, blk, None, None),
        P(grp, blk),
        P(grp, blk),
    )
    return jax.shard_map(shards, mesh=finer, in_specs=placed, out_specs=(P(both), P(both), P()), check_vma=False)
```

```python
import jax
import jax.numpy as jnp
from jax import lax
from jax.experimental import pallas as pl
from jax.experimental.pallas import tpu as pltpu
from jax.sharding import Mesh
from jax.sharding import PartitionSpec as P

F32 = jnp.float32
BF16 = jnp.bfloat16
MESH = pl.DeviceIdType.MESH
EPSILON = 1e-06
STEP_SCALE = 0.5
FAR = 1e30


def halves(v):
    hi = v.astype(BF16)
    mid = (v - hi.astype(F32)).astype(BF16)
    return jnp.concatenate([hi, mid], axis=1)


def pick(onehot, pair):
    both = jnp.dot(onehot, pair, preferred_element_type=F32)
    return both[:, 0:128] + both[:, 128:256]


def onehot(cond):
    return jnp.where(cond, 1.0, 0.0).astype(BF16)


def iota(shape, dim):
    return lax.broadcasted_iota(jnp.int32, shape, dim)


def folded(v):
    return jnp.sum(v.reshape(-1, 8, 128), axis=0)


def scalar_sum(v):
    return jnp.sum(jnp.sum(v, axis=0, keepdims=True), axis=1, keepdims=True)


def kernel(
    x_h, y_h, c_h, lo_h, hi_h, bk_h, b_h, rk_h, q_h, k_h, qi_h, kr_h, kc_h,
    xo_h, yo_h, w_s,
    tiles, bounds, kinds, rkind, hz, sh, hr, nidp, selp,
    xpl, cpl, y0, rows, idz, idp, idg, nid, sel, es, eo, ed, ysel,
    sx, xr, sc, cr, xs, cst, yrows, ys, kp, zprod, sps, spo, gps, gpo, dbuf, wz, wp,
    qi_s, kr_s, kc_s, loc, zs, zr, ps, pr, gs, gr, ws, wr,
):
    z = lax.axis_index("z")
    px, py = lax.axis_index("x"), lax.axis_index("yl")
    gh, gl = lax.axis_index("yh"), lax.axis_index("co")
    p, g = px * 2 + py, gh * 2 + gl
    pending = []

    def z_peer(k):
        return {"z": lax.rem(z + k, 8)}

    def p_peer(k):
        return {"x": lax.rem(px + k // 2, 4), "yl": lax.rem(py + k % 2, 2)}

    def g_peer(k):
        return {"yh": lax.rem(gh + k // 2, 2), "co": lax.rem(gl + k % 2, 2)}

    def w_peer(k):
        return {**p_peer(k // 4), **g_peer(k % 4)}

    def p_index(k):
        return lax.rem(px + k // 2, 4) * 2 + lax.rem(py + k % 2, 2)

    barrier = pltpu.get_barrier_semaphore()
    for k in range(1, 8):
        pl.semaphore_signal(barrier, inc=1, device_id=z_peer(k), device_id_type=MESH)
    for k in range(1, 32):
        pl.semaphore_signal(barrier, inc=1, device_id=w_peer(k), device_id_type=MESH)

    def load(n, *pairs):
        for src, dst in pairs:
            pltpu.make_async_copy(src, dst, loc.at[n]).start()

    def loaded(n, part):
        pltpu.make_async_copy(part, part, loc.at[n]).wait()

    index_loads = [
        pltpu.make_async_copy(src, dst, loc.at[n])
        for n, (src, dst) in enumerate(((qi_h, qi_s), (kr_h, kr_s), (kc_h, kc_s)))
    ]
    for copy in index_loads:
        copy.start()
    load(3, (x_h, xpl.at[p]))
    load(4, (y_h, y0.at[g]))
    load(5, (c_h, cpl.at[0, p]), (lo_h, bounds.at[0]), (hi_h, bounds.at[1]), (bk_h, kinds))
    load(6, (b_h, rows.at[g, 0]), (rk_h, rkind))
    load(7, *((k_h.at[0, t], tiles.at[4 + t]) for t in range(6)))
    load(8, *((q_h.at[0, t], tiles.at[t]) for t in range(4)))

    def send(count, peer, ssem, rsem, stage, source, target, whole):
        for k in range(1, count):
            pltpu.make_async_remote_copy(
                src_ref=source(k), dst_ref=target, send_sem=ssem.at[stage], recv_sem=rsem.at[stage],
                device_id=peer(k), device_id_type=MESH,
            ).start()
        pending.append((whole, ssem.at[stage]))
        return whole, rsem.at[stage]

    def send_z(stage, source, target, whole):
        return send(8, z_peer, zs, zr, stage, source, target, whole)

    def send_p(stage, source, target, whole):
        return send(8, p_peer, ps, pr, stage, source, target, whole)

    def send_g(stage, source, target, whole):
        return send(4, g_peer, gs, gr, stage, source, target, whole)

    def send_w(stage, source, target, whole):
        return send(32, w_peer, ws, wr, stage, source, target, whole)

    def arrive(stage):
        whole, sem = stage
        pltpu.make_async_copy(whole, whole, sem).wait()

    lane, sub = iota((4, 128), 1), iota((4, 128), 0)
    sub8 = iota((8, 128), 0)

    def ids_at(place, ids):
        slot = place // 4
        value = jnp.zeros((4, 128), jnp.int32)
        for n, scalar in enumerate(ids):
            value = jnp.where(slot == n, scalar, value)
        return jnp.where((place >= 0) & (place < 4 * len(ids)), value * 4 + place % 4 + 1, 0)

    for copy in index_loads:
        copy.wait()
    cons_cols = [kc_s[0, t] for t in range(6)]
    sent_v = ids_at(lane - lax.rem(z, 2) * 64, [qi_s[0, 0, t] for t in range(4)] + cons_cols)
    need_v = ids_at(lane, [qi_s[0, 1, t] for t in range(4)] + cons_cols)
    rows_v = ids_at(lane - g * 24, [kr_s[0, t] for t in range(6)])
    ids = jnp.where(sub == 0, sent_v, jnp.where(sub == 1, need_v, jnp.where(sub == 2, rows_v, 0))).astype(F32)
    idz[z] = ids
    idp[p] = ids
    idg[g] = ids
    for zz in range(8):
        zprod[0, zz, 40:64, :] = jnp.zeros((24, 128), F32)
        zprod[1, zz, 40:64, :] = jnp.zeros((24, 128), F32)

    pl.semaphore_wait(barrier, 38)

    id_z = send_z(0, lambda k: idz.at[z], idz.at[z], idz.at[pl.ds(0, 7)])
    loaded(3, x_h)
    x_plane = send_p(0, lambda k: xpl.at[p], xpl.at[p], xpl.at[pl.ds(0, 7)])
    id_g = send_g(0, lambda k: idg.at[g], idg.at[g], idg.at[pl.ds(0, 3)])
    id_p = send_p(1, lambda k: idp.at[p], idp.at[p], idp.at[pl.ds(0, 7)])
    loaded(4, y_h)
    y_all = send_g(1, lambda k: y0.at[g], y0.at[g], y0.at[pl.ds(0, 3)])
    loaded(5, cpl.at[0, pl.ds(0, 4)])
    kind = kinds[...]
    cpl[1, p] = jnp.where((kind == 1) | (kind == 2), bounds[0], -FAR)
    upper = jnp.where((kind == 2) | (kind == 3), bounds[1], FAR)
    hz[z] = upper
    hi_line = send_z(4, lambda k: hz.at[z], hz.at[z], hz.at[pl.ds(0, 7)])
    cst[2, 0:64, :] = upper
    loaded(6, rows.at[0])
    rows[g, 1] = rkind[...].astype(F32)
    xs[0, 0:64, :] = xpl[p]

    eye40 = iota((40, 128), 0) == iota((40, 128), 1)

    def column(row, mask):
        return jnp.sum(jnp.where(mask, row, 0.0), axis=1, keepdims=True)

    arrive(id_z)
    c_plane = [send_p(2 + a, lambda k: cpl.at[a, p], cpl.at[a, p], cpl.at[a, pl.ds(0, 7)]) for a in range(2)]
    rows_all = send_g(2, lambda k: rows.at[g], rows.at[g], rows.at[pl.ds(0, 3)])
    for zz in range(8):
        nid[40 * zz : 40 * zz + 40, :] = jnp.broadcast_to(column(idz[zz, 1:2, :], eye40), (40, 128))
    for n in range(4):
        have = (z * 512 + n * 128 + 1 + iota((1, 128), 1)).astype(F32)
        sel[:, n * 128 : (n + 1) * 128] = onehot(nid[...] == have)

    arrive(x_plane)
    sx[...] = pick(sel[...], halves(xpl[...].reshape(512, 128))).reshape(8, 40, 128)
    xr[z] = sx[z]
    x_slots = send_z(1, lambda k: sx.at[lax.rem(z + k, 8)], xr.at[z], xr.at[pl.ds(0, 7)])

    eye = iota((128, 128), 0) == iota((128, 128), 1)

    def forward(first, pairs, source, store):
        def body(i, _):
            x8 = source(i)
            out = jnp.zeros((8, 128), F32)
            for h in range(2):
                for r in range(4):
                    total = None
                    for n in range(4):
                        part = tiles[first + 2 * i + h, r * 128 : (r + 1) * 128, n * 128 : (n + 1) * 128]
                        part = part * x8[4 * h + n : 4 * h + n + 1, :]
                        total = part if total is None else total + part
                    col = jnp.sum(total, axis=1, keepdims=True)
                    row = jnp.sum(jnp.where(eye, col, 0.0), axis=0, keepdims=True)
                    out = jnp.where(sub8 == 4 * h + r, row, out)
            store(i, out)
            return 0

        lax.fori_loop(0, pairs, body, 0)

    def transposed(stage):
        def body(i, _):
            y8 = yrows[pl.ds(pl.multiple_of(8 * i, 8), 8), :]
            out = jnp.zeros((8, 128), F32)
            for h in range(2):
                totals = [None] * 4
                for r in range(4):
                    col = column(y8[4 * h + r : 4 * h + r + 1, :], eye)
                    for n in range(4):
                        part = tiles[4 + 2 * i + h, r * 128 : (r + 1) * 128, n * 128 : (n + 1) * 128]
                        part = folded(part * col)
                        totals[n] = part if totals[n] is None else totals[n] + part
                for n in range(4):
                    row = jnp.sum(totals[n], axis=0, keepdims=True)
                    out = jnp.where(sub8 == 4 * h + n, row, out)
            zprod[stage, z, pl.ds(pl.multiple_of(16 + 8 * i, 8), 8), :] = -out
            return 0

        lax.fori_loop(0, 3, body, 0)

    def hess(step):
        def source(i):
            return xs[step, pl.ds(pl.multiple_of(64 + 8 * i, 8), 8), :]

        def store(i, out):
            zprod[step, z, pl.ds(pl.multiple_of(8 * i, 8), 8), :] = out

        forward(0, 2, source, store)

    def cons(step):
        def source(i):
            return xs[step, pl.ds(pl.multiple_of(80 + 8 * i, 8), 8), :]

        def store(i, out):
            kp[step, pl.ds(pl.multiple_of(8 * i, 8), 8), :] = out

        forward(4, 3, source, store)

    def send_products(stage, step, first, count):
        part = zprod.at[step, z, pl.ds(first, count)]
        return send_z(stage, lambda k: part, part, zprod.at[step, pl.ds(0, 7), pl.ds(first, count)])

    def picked(a):
        arrive(c_plane[a])
        sc[a] = pick(sel[...], halves(cpl[a].reshape(512, 128))).reshape(8, 40, 128)
        cr[a, z] = sc[a, z]
        cst[a, 0:64, :] = cpl[a, p]

    def send_constants(stage, a, n, first, count):
        return send_z(
            stage,
            lambda k: sc.at[pl.ds(a, n), lax.rem(z + k, 8), pl.ds(first, count)],
            cr.at[pl.ds(a, n), z, pl.ds(first, count)],
            cr.at[pl.ds(a, n), pl.ds(0, 7), pl.ds(first, count)],
        )

    arrive(id_g)
    eye32 = (iota((32, 128), 1) == iota((32, 128), 0) + g * 24) & (iota((32, 128), 0) < 24)
    ysel[...] = onehot(column(idg[g, 2:3, :], eye32) == (iota((32, 128), 1) + 1).astype(F32))
    arrive(y_all)
    ys[0] = y0[...].reshape(128, 128)
    loaded(7, tiles.at[pl.ds(0, 6)])
    yrows[...] = pick(ysel[...], halves(ys[0]))
    transposed(0)
    products = [send_products(10, 0, 16, 24)]

    arrive(id_p)
    for pp in range(8):
        nidp[40 * pp : 40 * pp + 40, :] = jnp.broadcast_to(column(idp[pp, 1:2, :], eye40), (40, 128))
    for n in range(4):
        at = n * 128 + iota((1, 128), 1)
        have = (((at // 64) * 8 + p) * 64 + at % 64 + 1).astype(F32)
        selp[:, n * 128 : (n + 1) * 128] = onehot(nidp[...] == have)
    arrive(hi_line)
    sh[...] = pick(selp[...], halves(hz[...].reshape(512, 128))).reshape(8, 40, 128)
    hr[p] = sh[p]
    hi_slots = send_p(9, lambda k: sh.at[p_index(k)], hr.at[p], hr.at[pl.ds(0, 7)])

    loaded(8, tiles.at[pl.ds(0, 4)])
    arrive(x_slots)
    xs[0, 64:104, :] = jnp.sum(xr[...], axis=0)
    hess(0)
    products.append(send_products(5, 0, 0, 16))

    picked(0)
    picked(1)

    own = (z * 512 + 1 + iota((512, 128), 0)).astype(F32)
    for n in range(4):
        made = idz[2 * n, 0:1, :] + idz[2 * n + 1, 0:1, :]
        es[:, n * 128 : (n + 1) * 128] = onehot(nidp[...] == made)
        eo[:, n * 128 : (n + 1) * 128] = onehot(own == made)
    all_rows = idg[0, 2:3, :] + idg[1, 2:3, :] + idg[2, 2:3, :] + idg[3, 2:3, :]
    ed[...] = onehot((iota((128, 128), 0) + 1).astype(F32) == all_rows)[:, 0:96]

    cons(0)
    cons_all = send_constants(2, 0, 2, 16, 24)

    def next_weight(stage, weight):
        sums = jnp.sum(wp[stage], axis=0)
        total = jnp.sum(sums, axis=1, keepdims=True) + EPSILON
        return jnp.sqrt(weight * jnp.sqrt(total[1:2] / total[0:1]))

    weight = jnp.ones((1, 1), F32)
    for step in range(2):
        for stage in products:
            arrive(stage)
        pair = halves(zprod[step].reshape(512, 128))
        sps[step] = pick(es[...], pair).reshape(8, 40, 128)
        gps[step, p] = sps[step, p]
        first = 16 * step
        grad_s = send_p(
            5 + 2 * step,
            lambda k: sps.at[step, p_index(k), pl.ds(first, 40 - first)],
            gps.at[step, p, pl.ds(first, 40 - first)],
            gps.at[step, pl.ds(0, 7), pl.ds(first, 40 - first)],
        )
        spo[step] = pick(eo[...], pair).reshape(8, 64, 128)
        gpo[step, p] = spo[step, p]
        if step == 0:
            hess_all = send_constants(3, 0, 2, 0, 16)
            arrive(hi_slots)
            cst[2, 64:104, :] = jnp.sum(hr[...], axis=0)
            arrive(cons_all)
            for a in range(2):
                cst[a, 80:104, :] = jnp.sum(cr[a, :, 16:40, :], axis=0)
        grad_o = send_p(6 + 2 * step, lambda k: spo.at[step, p_index(k)], gpo.at[step, p], gpo.at[step, pl.ds(0, 7)])
        if step == 1:
            arrive(w_p)
            weight = next_weight(0, weight)
        step_primal = STEP_SCALE / weight
        step_dual = STEP_SCALE * weight

        def advance(a, b, total):
            here = pl.ds(a, b - a)
            current = xs[step, here, :]
            moved = current - step_primal * (total + cst[0, here, :])
            updated = jnp.minimum(jnp.maximum(moved, cst[1, here, :]), cst[2, here, :])
            xs[step + 1, here, :] = updated
            return updated - current

        arrive(grad_s)
        advance(80, 104, jnp.sum(gps[step, :, 16:40, :], axis=0))

        cons(step + 1)
        dbuf[step, g] = 2.0 * kp[step + 1] - kp[step]
        duals_g = send_g(3 + step, lambda k: dbuf.at[step, g], dbuf.at[step, g], dbuf.at[step, pl.ds(0, 3)])
        if step == 0:
            arrive(hess_all)
            for a in range(2):
                cst[a, 64:80, :] = jnp.sum(cr[a, :, 0:16, :], axis=0)
            advance(64, 80, jnp.sum(gps[0, :, 0:16, :], axis=0))
            hess(1)
            products = [send_products(6, 1, 0, 16)]
            arrive(rows_all)
        arrive(grad_o)
        moved = advance(0, 64, jnp.sum(gpo[step], axis=0))
        wz[step, z, 0:1, :] = jnp.sum(moved * moved, axis=0, keepdims=True)
        if step == 1:
            x_out = pltpu.make_async_copy(xs.at[2, pl.ds(0, 64)], xo_h, loc.at[9])
            x_out.start()
        arrive(duals_g)
        extrap = pick(ed[...], halves(dbuf[step].reshape(96, 128)))
        duals = ys[step]
        dual_new = duals + step_dual * (rows[:, 0].reshape(128, 128) - extrap)
        dual_new = jnp.where(rows[:, 1].reshape(128, 128) == 1.0, jnp.maximum(dual_new, 0.0), dual_new)
        ys[step + 1] = dual_new
        moved = dual_new - duals
        wz[step, z, 1:2, :] = jnp.sum(moved * moved, axis=0, keepdims=True) * 0.25
        w_z = send_z(8 + step, lambda k: wz.at[step, z], wz.at[step, z], wz.at[step, pl.ds(0, 7)])
        if step == 0:
            yrows[...] = pick(ysel[...], halves(dual_new))
            transposed(1)
            products.append(send_products(7, 1, 16, 24))
        if step == 1:
            y_out = pltpu.make_async_copy(ys.at[2, pl.ds(pl.multiple_of(g * 32, 32), 32)], yo_h, loc.at[10])
            y_out.start()
        arrive(w_z)
        wp[step, p * 4 + g] = jnp.sum(wz[step], axis=0)
        w_p = send_w(step, lambda k: wp.at[step, p * 4 + g], wp.at[step, p * 4 + g], wp.at[step, pl.ds(0, 31)])

    arrive(w_p)
    w_s[0, 0] = next_weight(1, weight)[0, 0]
    x_out.wait()
    y_out.wait()
    for stage in pending:
        arrive(stage)


def shards(primal, dual, objective, lower, upper, bound_kind, rhs, row_kind, q_tiles, q_index, k_tiles, k_rows, k_cols):
    hbm = pl.BlockSpec(memory_space=pl.ANY)
    anywhere = pl.BlockSpec(memory_space=pl.ANY)
    smem = pl.BlockSpec(memory_space=pltpu.SMEM)
    vmem, dma = pltpu.VMEM, pltpu.SemaphoreType.DMA

    def lines(v):
        return v.reshape(-1, 128)

    final_x, final_y, weight = pl.pallas_call(
        kernel,
        name="pdhg",
        out_shape=(
            jax.ShapeDtypeStruct((64, 128), F32),
            jax.ShapeDtypeStruct((32, 128), F32),
            jax.ShapeDtypeStruct((1, 1), F32),
        ),
        in_specs=[hbm] * 13,
        out_specs=(anywhere, anywhere, smem),
        scratch_shapes=[
            vmem((10, 512, 512), F32),
            vmem((2, 64, 128), F32),
            vmem((64, 128), jnp.int32),
            vmem((32, 128), jnp.int32),
            vmem((8, 64, 128), F32),
            vmem((8, 40, 128), F32),
            vmem((8, 40, 128), F32),
            vmem((320, 128), F32),
            vmem((320, 512), BF16),
            vmem((8, 64, 128), F32),
            vmem((2, 8, 64, 128), F32),
            vmem((4, 32, 128), F32),
            vmem((4, 2, 32, 128), F32),
            vmem((8, 4, 128), F32),
            vmem((8, 4, 128), F32),
            vmem((4, 4, 128), F32),
            vmem((320, 128), F32),
            vmem((320, 512), BF16),
            vmem((320, 512), BF16),
            vmem((512, 512), BF16),
            vmem((128, 96), BF16),
            vmem((32, 128), BF16),
            vmem((8, 40, 128), F32),
            vmem((8, 40, 128), F32),
            vmem((2, 8, 40, 128), F32),
            vmem((2, 8, 40, 128), F32),
            vmem((3, 104, 128), F32),
            vmem((3, 104, 128), F32),
            vmem((32, 128), F32),
            vmem((3, 128, 128), F32),
            vmem((3, 24, 128), F32),
            vmem((2, 8, 64, 128), F32),
            vmem((2, 8, 40, 128), F32),
            vmem((2, 8, 64, 128), F32),
            vmem((2, 8, 40, 128), F32),
            vmem((2, 8, 64, 128), F32),
            vmem((2, 4, 24, 128), F32),
            vmem((2, 8, 2, 128), F32),
            vmem((2, 32, 2, 128), F32),
            pltpu.SMEM((1, 2, 4), jnp.int32),
            pltpu.SMEM((1, 6), jnp.int32),
            pltpu.SMEM((1, 6), jnp.int32),
            dma((11,)),
            dma((11,)),
            dma((11,)),
            dma((10,)),
            dma((10,)),
            dma((5,)),
            dma((5,)),
            dma((2,)),
            dma((2,)),
        ],
        compiler_params=pltpu.CompilerParams(
            collective_id=0, has_side_effects=True, vmem_limit_bytes=67043328
        ),
    )(
        lines(primal), lines(dual), lines(objective), lines(lower), lines(upper), lines(bound_kind),
        lines(rhs), lines(row_kind), q_tiles, k_tiles, q_index, k_rows, k_cols,
    )
    return final_x.reshape(-1), final_y.reshape(-1), weight.reshape(())


def solution(mesh):
    finer = Mesh(mesh.devices.reshape(2, 2, 8, 4, 2), ("yh", "co", "z", "x", "yl"))
    grp, blk, both = ("yh", "co"), ("z", "x", "yl"), ("z", "x", "yl", "yh", "co")
    placed = (P(both),) * 8 + (
        P(grp, blk, None, None),
        P(grp, None, blk),
        P(grp, blk, None, None),
        P(grp, blk),
        P(grp, blk),
    )
    return jax.shard_map(shards, mesh=finer, in_specs=placed, out_specs=(P(both), P(both), P()), check_vma=False)
```

```python
import jax
import jax.numpy as jnp
from jax import lax
from jax.experimental import pallas as pl
from jax.experimental.pallas import tpu as pltpu
from jax.sharding import Mesh
from jax.sharding import PartitionSpec as P

F32 = jnp.float32
BF16 = jnp.bfloat16
MESH = pl.DeviceIdType.MESH
EPSILON = 1e-06
STEP_SCALE = 0.5
FAR = 1e30


def halves(v):
    hi = v.astype(BF16)
    mid = (v - hi.astype(F32)).astype(BF16)
    return jnp.concatenate([hi, mid], axis=1)


def pick(onehot, pair):
    both = jnp.dot(onehot, pair, preferred_element_type=F32)
    return both[:, 0:128] + both[:, 128:256]


def onehot(cond):
    return jnp.where(cond, 1.0, 0.0).astype(BF16)


def iota(shape, dim):
    return lax.broadcasted_iota(jnp.int32, shape, dim)


def folded(v):
    return jnp.sum(v.reshape(-1, 8, 128), axis=0)


def scalar_sum(v):
    return jnp.sum(jnp.sum(v, axis=0, keepdims=True), axis=1, keepdims=True)


def kernel(
    x_h, y_h, c_h, lo_h, hi_h, bk_h, b_h, rk_h, q_h, k_h, qi_h, kr_h, kc_h,
    xo, yo, w_s,
    tiles, bounds, kinds, rkind, hz, sh, hr, nidp, selp,
    xpl, cpl, y0, rows, idz, idp, idg, nid, sel, es, eo, ed, ysel,
    sx, xr, sc, cr, xs, cst, yrows, ys, kp, zprod, sps, spo, gps, gpo, dbuf, wz, wp, wg,
    qi_s, kr_s, kc_s, loc, zs, zr, ps, pr, gs, gr,
):
    z = lax.axis_index("z")
    px, py = lax.axis_index("x"), lax.axis_index("yl")
    gh, gl = lax.axis_index("yh"), lax.axis_index("co")
    p, g = px * 2 + py, gh * 2 + gl
    pending = []

    def z_peer(k):
        return {"z": lax.rem(z + k, 8)}

    def p_peer(k):
        return {"x": lax.rem(px + k // 2, 4), "yl": lax.rem(py + k % 2, 2)}

    def g_peer(k):
        return {"yh": lax.rem(gh + k // 2, 2), "co": lax.rem(gl + k % 2, 2)}

    def p_index(k):
        return lax.rem(px + k // 2, 4) * 2 + lax.rem(py + k % 2, 2)

    barrier = pltpu.get_barrier_semaphore()
    for k in range(1, 8):
        pl.semaphore_signal(barrier, inc=1, device_id=z_peer(k), device_id_type=MESH)
        pl.semaphore_signal(barrier, inc=1, device_id=p_peer(k), device_id_type=MESH)
    for k in range(1, 4):
        pl.semaphore_signal(barrier, inc=1, device_id=g_peer(k), device_id_type=MESH)

    def load(n, *pairs):
        for src, dst in pairs:
            pltpu.make_async_copy(src, dst, loc.at[n]).start()

    def loaded(n, part):
        pltpu.make_async_copy(part, part, loc.at[n]).wait()

    index_loads = [
        pltpu.make_async_copy(src, dst, loc.at[n])
        for n, (src, dst) in enumerate(((qi_h, qi_s), (kr_h, kr_s), (kc_h, kc_s)))
    ]
    for copy in index_loads:
        copy.start()
    load(3, (x_h, xpl.at[p]))
    load(4, (y_h, y0.at[g]))
    load(5, (c_h, cpl.at[0, p]), (lo_h, bounds.at[0]), (hi_h, bounds.at[1]), (bk_h, kinds))
    load(6, (b_h, rows.at[g, 0]), (rk_h, rkind))
    load(7, *((k_h.at[0, t], tiles.at[4 + t]) for t in range(6)))
    load(8, *((q_h.at[0, t], tiles.at[t]) for t in range(4)))

    def send(count, peer, ssem, rsem, stage, source, target, whole):
        for k in range(1, count):
            pltpu.make_async_remote_copy(
                src_ref=source(k), dst_ref=target, send_sem=ssem.at[stage], recv_sem=rsem.at[stage],
                device_id=peer(k), device_id_type=MESH,
            ).start()
        pending.append((whole, ssem.at[stage]))
        return whole, rsem.at[stage]

    def send_z(stage, source, target, whole):
        return send(8, z_peer, zs, zr, stage, source, target, whole)

    def send_p(stage, source, target, whole):
        return send(8, p_peer, ps, pr, stage, source, target, whole)

    def send_g(stage, source, target, whole):
        return send(4, g_peer, gs, gr, stage, source, target, whole)

    def arrive(stage):
        whole, sem = stage
        pltpu.make_async_copy(whole, whole, sem).wait()

    lane, sub = iota((4, 128), 1), iota((4, 128), 0)
    sub8 = iota((8, 128), 0)

    def ids_at(place, ids):
        slot = place // 4
        value = jnp.zeros((4, 128), jnp.int32)
        for n, scalar in enumerate(ids):
            value = jnp.where(slot == n, scalar, value)
        return jnp.where((place >= 0) & (place < 4 * len(ids)), value * 4 + place % 4 + 1, 0)

    for copy in index_loads:
        copy.wait()
    cons_cols = [kc_s[0, t] for t in range(6)]
    sent_v = ids_at(lane - lax.rem(z, 2) * 64, [qi_s[0, 0, t] for t in range(4)] + cons_cols)
    need_v = ids_at(lane, [qi_s[0, 1, t] for t in range(4)] + cons_cols)
    rows_v = ids_at(lane - g * 24, [kr_s[0, t] for t in range(6)])
    ids = jnp.where(sub == 0, sent_v, jnp.where(sub == 1, need_v, jnp.where(sub == 2, rows_v, 0))).astype(F32)
    idz[z] = ids
    idp[p] = ids
    idg[g] = ids
    for zz in range(8):
        zprod[0, zz, 40:64, :] = jnp.zeros((24, 128), F32)
        zprod[1, zz, 40:64, :] = jnp.zeros((24, 128), F32)

    pl.semaphore_wait(barrier, 17)

    id_z = send_z(0, lambda k: idz.at[z], idz.at[z], idz.at[pl.ds(0, 7)])
    loaded(3, x_h)
    x_plane = send_p(0, lambda k: xpl.at[p], xpl.at[p], xpl.at[pl.ds(0, 7)])
    id_g = send_g(0, lambda k: idg.at[g], idg.at[g], idg.at[pl.ds(0, 3)])
    id_p = send_p(1, lambda k: idp.at[p], idp.at[p], idp.at[pl.ds(0, 7)])
    loaded(4, y_h)
    y_all = send_g(1, lambda k: y0.at[g], y0.at[g], y0.at[pl.ds(0, 3)])
    loaded(5, cpl.at[0, pl.ds(0, 4)])
    kind = kinds[...]
    cpl[1, p] = jnp.where((kind == 1) | (kind == 2), bounds[0], -FAR)
    upper = jnp.where((kind == 2) | (kind == 3), bounds[1], FAR)
    hz[z] = upper
    hi_line = send_z(4, lambda k: hz.at[z], hz.at[z], hz.at[pl.ds(0, 7)])
    cst[2, 0:64, :] = upper
    loaded(6, rows.at[0])
    rows[g, 1] = rkind[...].astype(F32)
    xs[0, 0:64, :] = xpl[p]

    eye40 = iota((40, 128), 0) == iota((40, 128), 1)

    def column(row, mask):
        return jnp.sum(jnp.where(mask, row, 0.0), axis=1, keepdims=True)

    arrive(id_z)
    c_plane = [send_p(2 + a, lambda k: cpl.at[a, p], cpl.at[a, p], cpl.at[a, pl.ds(0, 7)]) for a in range(2)]
    rows_all = send_g(2, lambda k: rows.at[g], rows.at[g], rows.at[pl.ds(0, 3)])
    for zz in range(8):
        nid[40 * zz : 40 * zz + 40, :] = jnp.broadcast_to(column(idz[zz, 1:2, :], eye40), (40, 128))
    for n in range(4):
        have = (z * 512 + n * 128 + 1 + iota((1, 128), 1)).astype(F32)
        sel[:, n * 128 : (n + 1) * 128] = onehot(nid[...] == have)

    arrive(x_plane)
    sx[...] = pick(sel[...], halves(xpl[...].reshape(512, 128))).reshape(8, 40, 128)
    xr[z] = sx[z]

    def send_x(stage, first, count):
        return send_z(
            stage,
            lambda k: sx.at[lax.rem(z + k, 8), pl.ds(first, count)],
            xr.at[z, pl.ds(first, count)],
            xr.at[pl.ds(0, 7), pl.ds(first, count)],
        )

    x_hess = send_x(1, 0, 16)

    eye = iota((128, 128), 0) == iota((128, 128), 1)

    def forward(first, pairs, source, store):
        def body(i, _):
            x8 = source(i)
            out = jnp.zeros((8, 128), F32)
            for h in range(2):
                for r in range(4):
                    total = None
                    for n in range(4):
                        part = tiles[first + 2 * i + h, r * 128 : (r + 1) * 128, n * 128 : (n + 1) * 128]
                        part = part * x8[4 * h + n : 4 * h + n + 1, :]
                        total = part if total is None else total + part
                    col = jnp.sum(total, axis=1, keepdims=True)
                    row = jnp.sum(jnp.where(eye, col, 0.0), axis=0, keepdims=True)
                    out = jnp.where(sub8 == 4 * h + r, row, out)
            store(i, out)
            return 0

        lax.fori_loop(0, pairs, body, 0, unroll=True)

    def transposed(stage):
        def body(i, _):
            y8 = yrows[pl.ds(pl.multiple_of(8 * i, 8), 8), :]
            out = jnp.zeros((8, 128), F32)
            for h in range(2):
                totals = [None] * 4
                for r in range(4):
                    col = column(y8[4 * h + r : 4 * h + r + 1, :], eye)
                    for n in range(4):
                        part = tiles[4 + 2 * i + h, r * 128 : (r + 1) * 128, n * 128 : (n + 1) * 128]
                        part = folded(part * col)
                        totals[n] = part if totals[n] is None else totals[n] + part
                for n in range(4):
                    row = jnp.sum(totals[n], axis=0, keepdims=True)
                    out = jnp.where(sub8 == 4 * h + n, row, out)
            zprod[stage, z, pl.ds(pl.multiple_of(16 + 8 * i, 8), 8), :] = -out
            return 0

        lax.fori_loop(0, 3, body, 0, unroll=True)

    def hess(step):
        def source(i):
            return xs[step, pl.ds(pl.multiple_of(64 + 8 * i, 8), 8), :]

        def store(i, out):
            zprod[step, z, pl.ds(pl.multiple_of(8 * i, 8), 8), :] = out

        forward(0, 2, source, store)

    def cons(step):
        def source(i):
            return xs[step, pl.ds(pl.multiple_of(80 + 8 * i, 8), 8), :]

        def store(i, out):
            kp[step, pl.ds(pl.multiple_of(8 * i, 8), 8), :] = out

        forward(4, 3, source, store)

    def send_products(stage, step, first, count):
        part = zprod.at[step, z, pl.ds(first, count)]
        return send_z(stage, lambda k: part, part, zprod.at[step, pl.ds(0, 7), pl.ds(first, count)])

    def picked(a):
        arrive(c_plane[a])
        sc[a] = pick(sel[...], halves(cpl[a].reshape(512, 128))).reshape(8, 40, 128)
        cr[a, z] = sc[a, z]
        cst[a, 0:64, :] = cpl[a, p]

    def send_constants(stage, a, n, first, count):
        return send_z(
            stage,
            lambda k: sc.at[pl.ds(a, n), lax.rem(z + k, 8), pl.ds(first, count)],
            cr.at[pl.ds(a, n), z, pl.ds(first, count)],
            cr.at[pl.ds(a, n), pl.ds(0, 7), pl.ds(first, count)],
        )

    arrive(id_g)
    eye32 = (iota((32, 128), 1) == iota((32, 128), 0) + g * 24) & (iota((32, 128), 0) < 24)
    ysel[...] = onehot(column(idg[g, 2:3, :], eye32) == (iota((32, 128), 1) + 1).astype(F32))
    arrive(y_all)
    ys[0] = y0[...].reshape(128, 128)
    loaded(7, tiles.at[pl.ds(0, 6)])
    yrows[...] = pick(ysel[...], halves(ys[0]))
    transposed(0)
    products = [send_products(10, 0, 16, 24)]
    x_cons = send_x(11, 16, 24)

    arrive(id_p)
    for pp in range(8):
        nidp[40 * pp : 40 * pp + 40, :] = jnp.broadcast_to(column(idp[pp, 1:2, :], eye40), (40, 128))
    for n in range(4):
        at = n * 128 + iota((1, 128), 1)
        have = (((at // 64) * 8 + p) * 64 + at % 64 + 1).astype(F32)
        selp[:, n * 128 : (n + 1) * 128] = onehot(nidp[...] == have)
    arrive(hi_line)
    sh[...] = pick(selp[...], halves(hz[...].reshape(512, 128))).reshape(8, 40, 128)
    hr[p] = sh[p]
    hi_slots = send_p(9, lambda k: sh.at[p_index(k)], hr.at[p], hr.at[pl.ds(0, 7)])

    loaded(8, tiles.at[pl.ds(0, 4)])
    arrive(x_hess)
    xs[0, 64:80, :] = jnp.sum(xr[:, 0:16, :], axis=0)
    hess(0)
    products.append(send_products(5, 0, 0, 16))

    picked(0)
    picked(1)

    own = (z * 512 + 1 + iota((512, 128), 0)).astype(F32)
    for n in range(4):
        made = idz[2 * n, 0:1, :] + idz[2 * n + 1, 0:1, :]
        es[:, n * 128 : (n + 1) * 128] = onehot(nidp[...] == made)
        eo[:, n * 128 : (n + 1) * 128] = onehot(own == made)
    all_rows = idg[0, 2:3, :] + idg[1, 2:3, :] + idg[2, 2:3, :] + idg[3, 2:3, :]
    ed[...] = onehot((iota((128, 128), 0) + 1).astype(F32) == all_rows)[:, 0:96]


    def next_weight(sums, weight):
        total = jnp.sum(sums, axis=1, keepdims=True) + EPSILON
        return jnp.sqrt(weight * jnp.sqrt(total[1:2] / total[0:1]))

    weight = jnp.ones((1, 1), F32)
    for step in range(2):
        arrive(products[0])
        if step == 0:
            cons_all = send_constants(2, 0, 2, 16, 24)
        arrive(products[1])
        pair = halves(zprod[step].reshape(512, 128))
        sps[step] = pick(es[...], pair).reshape(8, 40, 128)
        gps[step, p] = sps[step, p]

        def send_slots(stage, first, count):
            return send_p(
                stage,
                lambda k: sps.at[step, p_index(k), pl.ds(first, count)],
                gps.at[step, p, pl.ds(first, count)],
                gps.at[step, pl.ds(0, 7), pl.ds(first, count)],
            )

        def send_own():
            return send_p(6 + 2 * step, lambda k: spo.at[step, p_index(k)], gpo.at[step, p], gpo.at[step, pl.ds(0, 7)])

        grad_s = send_slots(5 + 2 * step, 16, 24)
        if step == 0:
            grad_h = send_slots(10, 0, 16)
        spo[step] = pick(eo[...], pair).reshape(8, 64, 128)
        gpo[step, p] = spo[step, p]
        if step == 0:
            arrive(x_cons)
            xs[0, 80:104, :] = jnp.sum(xr[:, 16:40, :], axis=0)
            cons(0)
            grad_o = send_own()
            hess_all = send_constants(3, 0, 2, 0, 16)
            arrive(hi_slots)
            cst[2, 64:104, :] = jnp.sum(hr[...], axis=0)
            arrive(cons_all)
            for a in range(2):
                cst[a, 80:104, :] = jnp.sum(cr[a, :, 16:40, :], axis=0)
        if step == 1:
            grad_o = send_own()
        if step == 1:
            arrive(w_p)
            weight = next_weight(jnp.sum(wp[0], axis=0), weight)
        step_primal = STEP_SCALE / weight
        step_dual = STEP_SCALE * weight

        def advance(a, b, total):
            here = pl.ds(a, b - a)
            current = xs[step, here, :]
            moved = current - step_primal * (total + cst[0, here, :])
            updated = jnp.minimum(jnp.maximum(moved, cst[1, here, :]), cst[2, here, :])
            xs[step + 1, here, :] = updated
            return updated - current

        arrive(grad_s)
        advance(80, 104, jnp.sum(gps[step, :, 16:40, :], axis=0))

        cons(step + 1)
        dbuf[step, g] = 2.0 * kp[step + 1] - kp[step]
        duals_g = send_g(3 + step, lambda k: dbuf.at[step, g], dbuf.at[step, g], dbuf.at[step, pl.ds(0, 3)])
        if step == 0:
            arrive(hess_all)
            arrive(grad_h)
            for a in range(2):
                cst[a, 64:80, :] = jnp.sum(cr[a, :, 0:16, :], axis=0)
            advance(64, 80, jnp.sum(gps[0, :, 0:16, :], axis=0))
            hess(1)
            products = [send_products(6, 1, 0, 16)]
            arrive(rows_all)
        arrive(grad_o)
        moved = advance(0, 64, jnp.sum(gpo[step], axis=0))
        wg[step, g] = jnp.sum(moved * moved, axis=0, keepdims=True)
        w_g = send_g(5 + step, lambda k: wg.at[step, g], wg.at[step, g], wg.at[step, pl.ds(0, 3)])
        if step == 1:
            xo[...] = xs[2, 0:64, :]
        arrive(duals_g)
        extrap = pick(ed[...], halves(dbuf[step].reshape(96, 128)))
        duals = ys[step]
        dual_new = duals + step_dual * (rows[:, 0].reshape(128, 128) - extrap)
        dual_new = jnp.where(rows[:, 1].reshape(128, 128) == 1.0, jnp.maximum(dual_new, 0.0), dual_new)
        ys[step + 1] = dual_new
        if step == 0:
            yrows[...] = pick(ysel[...], halves(dual_new))
            transposed(1)
            products.append(send_products(7, 1, 16, 24))
        else:
            yo[...] = ys[2, pl.ds(pl.multiple_of(g * 32, 32), 32), :]
        moved = dual_new - duals
        wz[step, z, 1:2, :] = jnp.sum(moved * moved, axis=0, keepdims=True)
        arrive(w_g)
        wz[step, z, 0:1, :] = jnp.sum(wg[step], axis=0)
        w_z = send_z(8 + step, lambda k: wz.at[step, z], wz.at[step, z], wz.at[step, pl.ds(0, 7)])
        arrive(w_z)
        wp[step, p] = jnp.sum(wz[step], axis=0)
        w_p = send_p((4, 11)[step], lambda k: wp.at[step, p], wp.at[step, p], wp.at[step, pl.ds(0, 7)])

    arrive(w_p)
    w_s[0, 0] = next_weight(jnp.sum(wp[1], axis=0), weight)[0, 0]
    for stage in pending:
        arrive(stage)


def shards(primal, dual, objective, lower, upper, bound_kind, rhs, row_kind, q_tiles, q_index, k_tiles, k_rows, k_cols):
    hbm = pl.BlockSpec(memory_space=pl.ANY)
    smem = pl.BlockSpec(memory_space=pltpu.SMEM)
    vmem, dma = pltpu.VMEM, pltpu.SemaphoreType.DMA

    def lines(v):
        return v.reshape(-1, 128)

    final_x, final_y, weight = pl.pallas_call(
        kernel,
        name="pdhg",
        out_shape=(
            vmem((64, 128), F32),
            vmem((32, 128), F32),
            jax.ShapeDtypeStruct((1, 1), F32),
        ),
        in_specs=[hbm] * 13,
        out_specs=(pl.BlockSpec(memory_space=vmem), pl.BlockSpec(memory_space=vmem), smem),
        scratch_shapes=[
            vmem((10, 512, 512), F32),
            vmem((2, 64, 128), F32),
            vmem((64, 128), jnp.int32),
            vmem((32, 128), jnp.int32),
            vmem((8, 64, 128), F32),
            vmem((8, 40, 128), F32),
            vmem((8, 40, 128), F32),
            vmem((320, 128), F32),
            vmem((320, 512), BF16),
            vmem((8, 64, 128), F32),
            vmem((2, 8, 64, 128), F32),
            vmem((4, 32, 128), F32),
            vmem((4, 2, 32, 128), F32),
            vmem((8, 4, 128), F32),
            vmem((8, 4, 128), F32),
            vmem((4, 4, 128), F32),
            vmem((320, 128), F32),
            vmem((320, 512), BF16),
            vmem((320, 512), BF16),
            vmem((512, 512), BF16),
            vmem((128, 96), BF16),
            vmem((32, 128), BF16),
            vmem((8, 40, 128), F32),
            vmem((8, 40, 128), F32),
            vmem((2, 8, 40, 128), F32),
            vmem((2, 8, 40, 128), F32),
            vmem((3, 104, 128), F32),
            vmem((3, 104, 128), F32),
            vmem((32, 128), F32),
            vmem((3, 128, 128), F32),
            vmem((3, 24, 128), F32),
            vmem((2, 8, 64, 128), F32),
            vmem((2, 8, 40, 128), F32),
            vmem((2, 8, 64, 128), F32),
            vmem((2, 8, 40, 128), F32),
            vmem((2, 8, 64, 128), F32),
            vmem((2, 4, 24, 128), F32),
            vmem((2, 8, 2, 128), F32),
            vmem((2, 8, 2, 128), F32),
            vmem((2, 4, 1, 128), F32),
            pltpu.SMEM((1, 2, 4), jnp.int32),
            pltpu.SMEM((1, 6), jnp.int32),
            pltpu.SMEM((1, 6), jnp.int32),
            dma((9,)),
            dma((12,)),
            dma((12,)),
            dma((12,)),
            dma((12,)),
            dma((7,)),
            dma((7,)),
        ],
        compiler_params=pltpu.CompilerParams(
            collective_id=0, has_side_effects=True, vmem_limit_bytes=67043328 - 128 * 1024
        ),
    )(
        lines(primal), lines(dual), lines(objective), lines(lower), lines(upper), lines(bound_kind),
        lines(rhs), lines(row_kind), q_tiles, k_tiles, q_index, k_rows, k_cols,
    )
    return final_x.reshape(-1), final_y.reshape(-1), weight.reshape(())


def solution(mesh):
    finer = Mesh(mesh.devices.reshape(2, 2, 8, 4, 2), ("yh", "co", "z", "x", "yl"))
    grp, blk, both = ("yh", "co"), ("z", "x", "yl"), ("z", "x", "yl", "yh", "co")
    placed = (P(both),) * 8 + (
        P(grp, blk, None, None),
        P(grp, None, blk),
        P(grp, blk, None, None),
        P(grp, blk),
        P(grp, blk),
    )
    return jax.shard_map(shards, mesh=finer, in_specs=placed, out_specs=(P(both), P(both), P()), check_vma=False)
```

```python
import jax
import jax.numpy as jnp
from jax import lax
from jax.experimental import pallas as pl
from jax.experimental.pallas import tpu as pltpu
from jax.sharding import Mesh
from jax.sharding import PartitionSpec as P

F32 = jnp.float32
BF16 = jnp.bfloat16
MESH = pl.DeviceIdType.MESH
EPSILON = 1e-06
STEP_SCALE = 0.5
FAR = 1e30
Z_ORDER = (4, 3, 5, 2, 6, 1, 7)
P_ORDER = (5, 4, 3, 7, 2, 6, 1)
G_ORDER = (3, 2, 1)


def halves(v):
    hi = v.astype(BF16)
    mid = (v - hi.astype(F32)).astype(BF16)
    return jnp.concatenate([hi, mid], axis=1)


def pick(onehot, pair):
    both = jnp.dot(onehot, pair, preferred_element_type=F32)
    return both[:, 0:128] + both[:, 128:256]


def onehot(cond):
    return jnp.where(cond, 1.0, 0.0).astype(BF16)


def iota(shape, dim):
    return lax.broadcasted_iota(jnp.int32, shape, dim)


def folded(v):
    return jnp.sum(v.reshape(-1, 8, 128), axis=0)


def scalar_sum(v):
    return jnp.sum(jnp.sum(v, axis=0, keepdims=True), axis=1, keepdims=True)


def kernel(
    x_h, y_h, c_h, lo_h, hi_h, bk_h, b_h, rk_h, q_h, k_h, qi_h, kr_h, kc_h,
    xo, yo, w_s,
    tiles, bounds, kinds, rkind, hz, sh, hr, nidp, selp,
    xpl, cpl, y0, rows, idz, idp, idg, nid, sel, es, eo, ed, ysel,
    sx, xr, sc, cr, xs, cst, yrows, ys, kp, zprod, sps, spo, gps, gpo, dbuf, wz, wp, wg,
    qi_s, kr_s, kc_s, loc, zs, zr, ps, pr, gs, gr,
):
    z = lax.axis_index("z")
    px, py = lax.axis_index("x"), lax.axis_index("yl")
    gh, gl = lax.axis_index("yh"), lax.axis_index("co")
    p, g = px * 2 + py, gh * 2 + gl
    pending = []

    def z_peer(k):
        return {"z": lax.rem(z + k, 8)}

    def p_peer(k):
        return {"x": lax.rem(px + k // 2, 4), "yl": lax.rem(py + k % 2, 2)}

    def g_peer(k):
        return {"yh": lax.rem(gh + k // 2, 2), "co": lax.rem(gl + k % 2, 2)}

    def p_index(k):
        return lax.rem(px + k // 2, 4) * 2 + lax.rem(py + k % 2, 2)

    barrier = pltpu.get_barrier_semaphore()
    for k in Z_ORDER:
        pl.semaphore_signal(barrier, inc=1, device_id=z_peer(k), device_id_type=MESH)
    for k in P_ORDER:
        pl.semaphore_signal(barrier, inc=1, device_id=p_peer(k), device_id_type=MESH)
    for k in G_ORDER:
        pl.semaphore_signal(barrier, inc=1, device_id=g_peer(k), device_id_type=MESH)

    def load(n, *pairs):
        for src, dst in pairs:
            pltpu.make_async_copy(src, dst, loc.at[n]).start()

    def loaded(n, part):
        pltpu.make_async_copy(part, part, loc.at[n]).wait()

    index_loads = [
        pltpu.make_async_copy(src, dst, loc.at[n])
        for n, (src, dst) in enumerate(((qi_h, qi_s), (kr_h, kr_s), (kc_h, kc_s)))
    ]
    for copy in index_loads:
        copy.start()
    load(3, (x_h, xpl.at[p]))
    load(4, (y_h, y0.at[g]))
    load(5, (c_h, cpl.at[0, p]), (lo_h, bounds.at[0]), (hi_h, bounds.at[1]), (bk_h, kinds))
    load(6, (b_h, rows.at[g, 0]), (rk_h, rkind))
    load(7, *((k_h.at[0, t], tiles.at[4 + t]) for t in range(6)))
    load(8, *((q_h.at[0, t], tiles.at[t]) for t in range(4)))

    def send(order, peer, ssem, rsem, stage, source, target, whole):
        for k in order:
            pltpu.make_async_remote_copy(
                src_ref=source(k), dst_ref=target, send_sem=ssem.at[stage], recv_sem=rsem.at[stage],
                device_id=peer(k), device_id_type=MESH,
            ).start()
        pending.append((whole, ssem.at[stage]))
        return whole, rsem.at[stage]

    def send_z(stage, source, target, whole):
        return send(Z_ORDER, z_peer, zs, zr, stage, source, target, whole)

    def send_p(stage, source, target, whole):
        return send(P_ORDER, p_peer, ps, pr, stage, source, target, whole)

    def send_g(stage, source, target, whole):
        return send(G_ORDER, g_peer, gs, gr, stage, source, target, whole)

    def arrive(stage):
        whole, sem = stage
        pltpu.make_async_copy(whole, whole, sem).wait()

    lane, sub = iota((4, 128), 1), iota((4, 128), 0)
    sub8 = iota((8, 128), 0)

    def ids_at(place, ids):
        slot = place // 4
        value = jnp.zeros((4, 128), jnp.int32)
        for n, scalar in enumerate(ids):
            value = jnp.where(slot == n, scalar, value)
        return jnp.where((place >= 0) & (place < 4 * len(ids)), value * 4 + place % 4 + 1, 0)

    for copy in index_loads:
        copy.wait()
    cons_cols = [kc_s[0, t] for t in range(6)]
    sent_v = ids_at(lane - lax.rem(z, 2) * 64, [qi_s[0, 0, t] for t in range(4)] + cons_cols)
    need_v = ids_at(lane, [qi_s[0, 1, t] for t in range(4)] + cons_cols)
    rows_v = ids_at(lane - g * 24, [kr_s[0, t] for t in range(6)])
    ids = jnp.where(sub == 0, sent_v, jnp.where(sub == 1, need_v, jnp.where(sub == 2, rows_v, 0))).astype(F32)
    idz[z] = ids
    idp[p] = ids
    idg[g] = ids
    for zz in range(8):
        zprod[0, zz, 40:64, :] = jnp.zeros((24, 128), F32)
        zprod[1, zz, 40:64, :] = jnp.zeros((24, 128), F32)

    pl.semaphore_wait(barrier, 17)

    id_z = send_z(0, lambda k: idz.at[z], idz.at[z], idz.at[pl.ds(0, 7)])
    loaded(3, x_h)
    x_plane = send_p(0, lambda k: xpl.at[p], xpl.at[p], xpl.at[pl.ds(0, 7)])
    id_g = send_g(0, lambda k: idg.at[g], idg.at[g], idg.at[pl.ds(0, 3)])
    id_p = send_p(1, lambda k: idp.at[p], idp.at[p], idp.at[pl.ds(0, 7)])
    loaded(4, y_h)
    y_all = send_g(1, lambda k: y0.at[g], y0.at[g], y0.at[pl.ds(0, 3)])
    loaded(5, cpl.at[0, pl.ds(0, 4)])
    kind = kinds[...]
    cpl[1, p] = jnp.where((kind == 1) | (kind == 2), bounds[0], -FAR)
    upper = jnp.where((kind == 2) | (kind == 3), bounds[1], FAR)
    hz[z] = upper
    hi_line = send_z(4, lambda k: hz.at[z], hz.at[z], hz.at[pl.ds(0, 7)])
    cst[2, 0:64, :] = upper
    loaded(6, rows.at[0])
    rows[g, 1] = rkind[...].astype(F32)
    xs[0, 0:64, :] = xpl[p]

    eye40 = iota((40, 128), 0) == iota((40, 128), 1)

    def column(row, mask):
        return jnp.sum(jnp.where(mask, row, 0.0), axis=1, keepdims=True)

    arrive(id_z)
    for zz in range(8):
        nid[40 * zz : 40 * zz + 40, :] = jnp.broadcast_to(column(idz[zz, 1:2, :], eye40), (40, 128))
    for n in range(4):
        have = (z * 512 + n * 128 + 1 + iota((1, 128), 1)).astype(F32)
        sel[:, n * 128 : (n + 1) * 128] = onehot(nid[...] == have)

    arrive(x_plane)
    sx[...] = pick(sel[...], halves(xpl[...].reshape(512, 128))).reshape(8, 40, 128)
    xr[z] = sx[z]

    def send_x(stage, first, count):
        return send_z(
            stage,
            lambda k: sx.at[lax.rem(z + k, 8), pl.ds(first, count)],
            xr.at[z, pl.ds(first, count)],
            xr.at[pl.ds(0, 7), pl.ds(first, count)],
        )

    x_hess = send_x(1, 0, 16)
    c_plane = [send_p(2 + a, lambda k: cpl.at[a, p], cpl.at[a, p], cpl.at[a, pl.ds(0, 7)]) for a in range(2)]
    rows_all = send_g(2, lambda k: rows.at[g], rows.at[g], rows.at[pl.ds(0, 3)])

    eye = iota((128, 128), 0) == iota((128, 128), 1)

    def forward(first, pairs, source, store):
        def body(i, _):
            x8 = source(i)
            out = jnp.zeros((8, 128), F32)
            for h in range(2):
                for r in range(4):
                    total = None
                    for n in range(4):
                        part = tiles[first + 2 * i + h, r * 128 : (r + 1) * 128, n * 128 : (n + 1) * 128]
                        part = part * x8[4 * h + n : 4 * h + n + 1, :]
                        total = part if total is None else total + part
                    col = jnp.sum(total, axis=1, keepdims=True)
                    row = jnp.sum(jnp.where(eye, col, 0.0), axis=0, keepdims=True)
                    out = jnp.where(sub8 == 4 * h + r, row, out)
            store(i, out)
            return 0

        lax.fori_loop(0, pairs, body, 0, unroll=True)

    def transposed(stage):
        def body(i, _):
            y8 = yrows[pl.ds(pl.multiple_of(8 * i, 8), 8), :]
            out = jnp.zeros((8, 128), F32)
            for h in range(2):
                totals = [None] * 4
                for r in range(4):
                    col = column(y8[4 * h + r : 4 * h + r + 1, :], eye)
                    for n in range(4):
                        part = tiles[4 + 2 * i + h, r * 128 : (r + 1) * 128, n * 128 : (n + 1) * 128]
                        part = folded(part * col)
                        totals[n] = part if totals[n] is None else totals[n] + part
                for n in range(4):
                    row = jnp.sum(totals[n], axis=0, keepdims=True)
                    out = jnp.where(sub8 == 4 * h + n, row, out)
            zprod[stage, z, pl.ds(pl.multiple_of(16 + 8 * i, 8), 8), :] = -out
            return 0

        lax.fori_loop(0, 3, body, 0, unroll=True)

    def hess(step):
        def source(i):
            return xs[step, pl.ds(pl.multiple_of(64 + 8 * i, 8), 8), :]

        def store(i, out):
            zprod[step, z, pl.ds(pl.multiple_of(8 * i, 8), 8), :] = out

        forward(0, 2, source, store)

    def cons(step):
        def source(i):
            return xs[step, pl.ds(pl.multiple_of(80 + 8 * i, 8), 8), :]

        def store(i, out):
            kp[step, pl.ds(pl.multiple_of(8 * i, 8), 8), :] = out

        forward(4, 3, source, store)

    def send_products(stage, step, first, count):
        part = zprod.at[step, z, pl.ds(first, count)]
        return send_z(stage, lambda k: part, part, zprod.at[step, pl.ds(0, 7), pl.ds(first, count)])

    def picked(a):
        arrive(c_plane[a])
        sc[a] = pick(sel[...], halves(cpl[a].reshape(512, 128))).reshape(8, 40, 128)
        cr[a, z] = sc[a, z]
        cst[a, 0:64, :] = cpl[a, p]

    def send_constants(stage, a, n, first, count):
        return send_z(
            stage,
            lambda k: sc.at[pl.ds(a, n), lax.rem(z + k, 8), pl.ds(first, count)],
            cr.at[pl.ds(a, n), z, pl.ds(first, count)],
            cr.at[pl.ds(a, n), pl.ds(0, 7), pl.ds(first, count)],
        )

    arrive(id_g)
    eye32 = (iota((32, 128), 1) == iota((32, 128), 0) + g * 24) & (iota((32, 128), 0) < 24)
    ysel[...] = onehot(column(idg[g, 2:3, :], eye32) == (iota((32, 128), 1) + 1).astype(F32))
    arrive(y_all)
    ys[0] = y0[...].reshape(128, 128)
    loaded(7, tiles.at[pl.ds(0, 6)])
    yrows[...] = pick(ysel[...], halves(ys[0]))
    transposed(0)
    products = [send_products(10, 0, 16, 24)]
    x_cons = send_x(11, 16, 24)

    arrive(id_p)
    for pp in range(8):
        nidp[40 * pp : 40 * pp + 40, :] = jnp.broadcast_to(column(idp[pp, 1:2, :], eye40), (40, 128))
    for n in range(4):
        at = n * 128 + iota((1, 128), 1)
        have = (((at // 64) * 8 + p) * 64 + at % 64 + 1).astype(F32)
        selp[:, n * 128 : (n + 1) * 128] = onehot(nidp[...] == have)
    arrive(hi_line)
    sh[...] = pick(selp[...], halves(hz[...].reshape(512, 128))).reshape(8, 40, 128)
    hr[p] = sh[p]
    hi_slots = send_p(9, lambda k: sh.at[p_index(k)], hr.at[p], hr.at[pl.ds(0, 7)])

    loaded(8, tiles.at[pl.ds(0, 4)])
    arrive(x_hess)
    xs[0, 64:80, :] = jnp.sum(xr[:, 0:16, :], axis=0)
    hess(0)
    products.append(send_products(5, 0, 0, 16))

    picked(0)
    picked(1)

    own = (z * 512 + 1 + iota((512, 128), 0)).astype(F32)
    for n in range(4):
        made = idz[2 * n, 0:1, :] + idz[2 * n + 1, 0:1, :]
        es[:, n * 128 : (n + 1) * 128] = onehot(nidp[...] == made)
        eo[:, n * 128 : (n + 1) * 128] = onehot(own == made)
    all_rows = idg[0, 2:3, :] + idg[1, 2:3, :] + idg[2, 2:3, :] + idg[3, 2:3, :]
    ed[...] = onehot((iota((128, 128), 0) + 1).astype(F32) == all_rows)[:, 0:96]


    def next_weight(sums, weight):
        total = jnp.sum(sums, axis=1, keepdims=True) + EPSILON
        return jnp.sqrt(weight * jnp.sqrt(total[1:2] / total[0:1]))

    weight = jnp.ones((1, 1), F32)
    for step in range(2):
        arrive(products[0])
        if step == 0:
            cons_all = send_constants(2, 0, 2, 16, 24)
        arrive(products[1])
        pair = halves(zprod[step].reshape(512, 128))
        sps[step] = pick(es[...], pair).reshape(8, 40, 128)
        gps[step, p] = sps[step, p]

        def send_slots(stage, first, count):
            return send_p(
                stage,
                lambda k: sps.at[step, p_index(k), pl.ds(first, count)],
                gps.at[step, p, pl.ds(first, count)],
                gps.at[step, pl.ds(0, 7), pl.ds(first, count)],
            )

        def send_own():
            return send_p(6 + 2 * step, lambda k: spo.at[step, p_index(k)], gpo.at[step, p], gpo.at[step, pl.ds(0, 7)])

        grad_s = send_slots(5 + 2 * step, 16, 24)
        spo[step] = pick(eo[...], pair).reshape(8, 64, 128)
        gpo[step, p] = spo[step, p]
        if step == 0:
            arrive(x_cons)
            xs[0, 80:104, :] = jnp.sum(xr[:, 16:40, :], axis=0)
            cons(0)
            grad_h = send_slots(10, 0, 16)
            grad_o = send_own()
            hess_all = send_constants(3, 0, 2, 0, 16)
            arrive(hi_slots)
            cst[2, 64:104, :] = jnp.sum(hr[...], axis=0)
            arrive(cons_all)
            for a in range(2):
                cst[a, 80:104, :] = jnp.sum(cr[a, :, 16:40, :], axis=0)
        if step == 1:
            grad_o = send_own()
        if step == 1:
            arrive(w_p)
            weight = next_weight(jnp.sum(wp[0], axis=0), weight)
        step_primal = STEP_SCALE / weight
        step_dual = STEP_SCALE * weight

        def advance(a, b, total):
            here = pl.ds(a, b - a)
            current = xs[step, here, :]
            moved = current - step_primal * (total + cst[0, here, :])
            updated = jnp.minimum(jnp.maximum(moved, cst[1, here, :]), cst[2, here, :])
            xs[step + 1, here, :] = updated
            return updated - current

        arrive(grad_s)
        advance(80, 104, jnp.sum(gps[step, :, 16:40, :], axis=0))

        cons(step + 1)
        dbuf[step, g] = 2.0 * kp[step + 1] - kp[step]
        duals_g = send_g(3 + step, lambda k: dbuf.at[step, g], dbuf.at[step, g], dbuf.at[step, pl.ds(0, 3)])
        if step == 0:
            arrive(hess_all)
            arrive(grad_h)
            for a in range(2):
                cst[a, 64:80, :] = jnp.sum(cr[a, :, 0:16, :], axis=0)
            advance(64, 80, jnp.sum(gps[0, :, 0:16, :], axis=0))
            hess(1)
            products = [send_products(6, 1, 0, 16)]
            arrive(rows_all)
        arrive(grad_o)
        moved = advance(0, 64, jnp.sum(gpo[step], axis=0))
        wg[step, g] = jnp.sum(moved * moved, axis=0, keepdims=True)
        w_g = send_g(5 + step, lambda k: wg.at[step, g], wg.at[step, g], wg.at[step, pl.ds(0, 3)])
        if step == 1:
            xo[...] = xs[2, 0:64, :]
        arrive(duals_g)
        extrap = pick(ed[...], halves(dbuf[step].reshape(96, 128)))
        duals = ys[step]
        dual_new = duals + step_dual * (rows[:, 0].reshape(128, 128) - extrap)
        dual_new = jnp.where(rows[:, 1].reshape(128, 128) == 1.0, jnp.maximum(dual_new, 0.0), dual_new)
        ys[step + 1] = dual_new
        if step == 0:
            yrows[...] = pick(ysel[...], halves(dual_new))
            transposed(1)
            products.append(send_products(7, 1, 16, 24))
        else:
            yo[...] = ys[2, pl.ds(pl.multiple_of(g * 32, 32), 32), :]
        moved = dual_new - duals
        wz[step, z, 1:2, :] = jnp.sum(moved * moved, axis=0, keepdims=True)
        arrive(w_g)
        wz[step, z, 0:1, :] = jnp.sum(wg[step], axis=0)
        w_z = send_z(8 + step, lambda k: wz.at[step, z], wz.at[step, z], wz.at[step, pl.ds(0, 7)])
        arrive(w_z)
        wp[step, p] = jnp.sum(wz[step], axis=0)
        w_p = send_p((4, 11)[step], lambda k: wp.at[step, p], wp.at[step, p], wp.at[step, pl.ds(0, 7)])

    arrive(w_p)
    w_s[0, 0] = next_weight(jnp.sum(wp[1], axis=0), weight)[0, 0]
    for stage in pending:
        arrive(stage)


def shards(primal, dual, objective, lower, upper, bound_kind, rhs, row_kind, q_tiles, q_index, k_tiles, k_rows, k_cols):
    hbm = pl.BlockSpec(memory_space=pl.ANY)
    smem = pl.BlockSpec(memory_space=pltpu.SMEM)
    vmem, dma = pltpu.VMEM, pltpu.SemaphoreType.DMA

    def lines(v):
        return v.reshape(-1, 128)

    final_x, final_y, weight = pl.pallas_call(
        kernel,
        name="pdhg",
        out_shape=(
            vmem((64, 128), F32),
            vmem((32, 128), F32),
            jax.ShapeDtypeStruct((1, 1), F32),
        ),
        in_specs=[hbm] * 13,
        out_specs=(pl.BlockSpec(memory_space=vmem), pl.BlockSpec(memory_space=vmem), smem),
        scratch_shapes=[
            vmem((10, 512, 512), F32),
            vmem((2, 64, 128), F32),
            vmem((64, 128), jnp.int32),
            vmem((32, 128), jnp.int32),
            vmem((8, 64, 128), F32),
            vmem((8, 40, 128), F32),
            vmem((8, 40, 128), F32),
            vmem((320, 128), F32),
            vmem((320, 512), BF16),
            vmem((8, 64, 128), F32),
            vmem((2, 8, 64, 128), F32),
            vmem((4, 32, 128), F32),
            vmem((4, 2, 32, 128), F32),
            vmem((8, 4, 128), F32),
            vmem((8, 4, 128), F32),
            vmem((4, 4, 128), F32),
            vmem((320, 128), F32),
            vmem((320, 512), BF16),
            vmem((320, 512), BF16),
            vmem((512, 512), BF16),
            vmem((128, 96), BF16),
            vmem((32, 128), BF16),
            vmem((8, 40, 128), F32),
            vmem((8, 40, 128), F32),
            vmem((2, 8, 40, 128), F32),
            vmem((2, 8, 40, 128), F32),
            vmem((3, 104, 128), F32),
            vmem((3, 104, 128), F32),
            vmem((32, 128), F32),
            vmem((3, 128, 128), F32),
            vmem((3, 24, 128), F32),
            vmem((2, 8, 64, 128), F32),
            vmem((2, 8, 40, 128), F32),
            vmem((2, 8, 64, 128), F32),
            vmem((2, 8, 40, 128), F32),
            vmem((2, 8, 64, 128), F32),
            vmem((2, 4, 24, 128), F32),
            vmem((2, 8, 2, 128), F32),
            vmem((2, 8, 2, 128), F32),
            vmem((2, 4, 1, 128), F32),
            pltpu.SMEM((1, 2, 4), jnp.int32),
            pltpu.SMEM((1, 6), jnp.int32),
            pltpu.SMEM((1, 6), jnp.int32),
            dma((9,)),
            dma((12,)),
            dma((12,)),
            dma((12,)),
            dma((12,)),
            dma((7,)),
            dma((7,)),
        ],
        compiler_params=pltpu.CompilerParams(
            collective_id=0, has_side_effects=True, vmem_limit_bytes=67043328 - 128 * 1024
        ),
    )(
        lines(primal), lines(dual), lines(objective), lines(lower), lines(upper), lines(bound_kind),
        lines(rhs), lines(row_kind), q_tiles, k_tiles, q_index, k_rows, k_cols,
    )
    return final_x.reshape(-1), final_y.reshape(-1), weight.reshape(())


def solution(mesh):
    finer = Mesh(mesh.devices.reshape(2, 2, 8, 4, 2), ("yh", "co", "z", "x", "yl"))
    grp, blk, both = ("yh", "co"), ("z", "x", "yl"), ("z", "x", "yl", "yh", "co")
    placed = (P(both),) * 8 + (
        P(grp, blk, None, None),
        P(grp, None, blk),
        P(grp, blk, None, None),
        P(grp, blk),
        P(grp, blk),
    )
    return jax.shard_map(shards, mesh=finer, in_specs=placed, out_specs=(P(both), P(both), P()), check_vma=False)
```

```python
import math

import jax
import jax.numpy as jnp
from jax import lax
from jax.experimental import pallas as pl
from jax.experimental.pallas import tpu as pltpu
from jax.sharding import Mesh
from jax.sharding import PartitionSpec as P

F32 = jnp.float32
BF16 = jnp.bfloat16
MESH = pl.DeviceIdType.MESH
EPSILON = 1e-06
STEP_SCALE = 0.5
FAR = 1e30
Z_ORDER = (4, 3, 5, 2, 6, 1, 7)
P_ORDER = (5, 4, 3, 7, 2, 6, 1)
OWN_ORDER = (5, 3, 7, 1, 4, 2, 6)
G_ORDER = (3, 2, 1)


def halves(v):
    hi = v.astype(BF16)
    mid = (v - hi.astype(F32)).astype(BF16)
    return jnp.concatenate([hi, mid], axis=1)


def pick(onehot, pair):
    both = jnp.dot(onehot, pair, preferred_element_type=F32)
    return both[:, 0:128] + both[:, 128:256]


def onehot(cond):
    return jnp.where(cond, 1.0, 0.0).astype(BF16)


def iota(shape, dim):
    return lax.broadcasted_iota(jnp.int32, shape, dim)


def folded(v):
    return jnp.sum(v.reshape(-1, 8, 128), axis=0)


def scalar_sum(v):
    return jnp.sum(jnp.sum(v, axis=0, keepdims=True), axis=1, keepdims=True)


def kernel(
    x_h, y_h, c_h, lo_h, hi_h, bk_h, b_h, rk_h, q_h, k_h, qi_h, kr_h, kc_h,
    xo, yo, w_s,
    tiles, bounds, kinds, rkind, hz, sh, hr, nidp, selp,
    xpl, cpl, y0, rows, idz, idp, idg, nid, selq, selk, esk, esq, eo, ed, ysel,
    sx, xr, sc, cr, xs, cst, yrows, ys, kp, zprod, spk, spq, spo, gpk, gpq, gpo, dbuf, wz, wp, wg,
    qi_s, kr_s, kc_s, lines, loc, ssems, zr, pr, gr,
):
    z = lax.axis_index("z")
    px, py = lax.axis_index("x"), lax.axis_index("yl")
    gh, gl = lax.axis_index("yh"), lax.axis_index("co")
    p, g = px * 2 + py, gh * 2 + gl
    sent = [0, 0, 0]

    def z_peer(k):
        return {"z": lax.rem(z + k, 8)}

    def p_peer(k):
        return {"x": lax.rem(px + k // 2, 4), "yl": lax.rem(py + k % 2, 2)}

    def g_peer(k):
        return {"yh": lax.rem(gh + k // 2, 2), "co": lax.rem(gl + k % 2, 2)}

    def p_index(k):
        return lax.rem(px + k // 2, 4) * 2 + lax.rem(py + k % 2, 2)

    barrier = pltpu.get_barrier_semaphore()
    for k in Z_ORDER:
        pl.semaphore_signal(barrier, inc=1, device_id=z_peer(k), device_id_type=MESH)
    for k in P_ORDER:
        pl.semaphore_signal(barrier, inc=1, device_id=p_peer(k), device_id_type=MESH)
    for k in G_ORDER:
        pl.semaphore_signal(barrier, inc=1, device_id=g_peer(k), device_id_type=MESH)

    def load(n, *pairs):
        for src, dst in pairs:
            pltpu.make_async_copy(src, dst, loc.at[n]).start()

    def loaded(n, part):
        pltpu.make_async_copy(part, part, loc.at[n]).wait()

    index_loads = [
        pltpu.make_async_copy(src, dst, loc.at[n])
        for n, (src, dst) in enumerate(((qi_h, qi_s), (kr_h, kr_s), (kc_h, kc_s)))
    ]
    for copy in index_loads:
        copy.start()
    load(3, (x_h, xpl.at[p]))
    load(4, (y_h, y0.at[g]))
    load(5, (c_h, cpl.at[0, p]), (lo_h, bounds.at[0]), (hi_h, bounds.at[1]), (bk_h, kinds))
    load(6, (b_h, rows.at[g, 0]), (rk_h, rkind))
    load(7, *((k_h.at[0, t], tiles.at[4 + t]) for t in range(6)))
    load(8, *((q_h.at[0, t], tiles.at[t]) for t in range(4)))

    def send(axis, order, peer, rsem, stage, source, target, whole):
        ssem = ssems.at[axis]
        for k in order:
            pltpu.make_async_remote_copy(
                src_ref=source(k), dst_ref=target, send_sem=ssem, recv_sem=rsem.at[stage],
                device_id=peer(k), device_id_type=MESH,
            ).start()
        sent[axis] += 4 * math.prod(whole.shape)
        return whole, rsem.at[stage]

    def send_z(stage, source, target, whole):
        return send(0, Z_ORDER, z_peer, zr, stage, source, target, whole)

    def send_p(stage, source, target, whole, order=P_ORDER):
        return send(1, order, p_peer, pr, stage, source, target, whole)

    def send_g(stage, source, target, whole):
        return send(2, G_ORDER, g_peer, gr, stage, source, target, whole)

    def arrive(stage):
        whole, sem = stage
        pltpu.make_async_copy(whole, whole, sem).wait()

    lane, sub = iota((4, 128), 1), iota((4, 128), 0)
    sub8 = iota((8, 128), 0)

    def ids_at(place, ids):
        slot = place // 4
        value = jnp.zeros((4, 128), jnp.int32)
        for n, scalar in enumerate(ids):
            value = jnp.where(slot == n, scalar, value)
        return jnp.where((place >= 0) & (place < 4 * len(ids)), value * 4 + place % 4 + 1, 0)

    for copy in index_loads:
        copy.wait()
    cons_cols = [kc_s[0, t] for t in range(6)]
    sent_v = ids_at(lane - lax.rem(z, 2) * 64, [qi_s[0, 0, t] for t in range(4)] + cons_cols)
    need_v = ids_at(lane, [qi_s[0, 1, t] for t in range(4)] + cons_cols)
    rows_v = ids_at(lane - g * 24, [kr_s[0, t] for t in range(6)])
    ids = jnp.where(sub == 0, sent_v, jnp.where(sub == 1, need_v, jnp.where(sub == 2, rows_v, 0))).astype(F32)
    idz[z] = ids
    idp[p] = ids
    idg[g] = ids
    for zz in range(8):
        zprod[0, zz, 40:64, :] = jnp.zeros((24, 128), F32)
        zprod[1, zz, 40:64, :] = jnp.zeros((24, 128), F32)

    pl.semaphore_wait(barrier, 17)

    id_z = send_z(0, lambda k: idz.at[z], idz.at[z], idz.at[pl.ds(0, 7)])
    loaded(3, x_h)
    x_plane = send_p(0, lambda k: xpl.at[p], xpl.at[p], xpl.at[pl.ds(0, 7)])
    id_g = send_g(0, lambda k: idg.at[g], idg.at[g], idg.at[pl.ds(0, 3)])
    id_p = send_p(1, lambda k: idp.at[p], idp.at[p], idp.at[pl.ds(0, 7)])
    loaded(4, y_h)
    y_all = send_g(1, lambda k: y0.at[g], y0.at[g], y0.at[pl.ds(0, 3)])
    loaded(5, cpl.at[0, pl.ds(0, 4)])
    kind = kinds[...]
    cpl[1, p] = jnp.where((kind == 1) | (kind == 2), bounds[0], -FAR)
    upper = jnp.where((kind == 2) | (kind == 3), bounds[1], FAR)
    hz[z] = upper
    hi_line = send_z(4, lambda k: hz.at[z], hz.at[z], hz.at[pl.ds(0, 7)])
    cst[2, 0:64, :] = upper
    loaded(6, rows.at[0])
    rows[g, 1] = rkind[...].astype(F32)
    xs[0, 0:64, :] = xpl[p]

    eye40 = iota((40, 128), 0) == iota((40, 128), 1)

    def column(row, mask):
        return jnp.sum(jnp.where(mask, row, 0.0), axis=1, keepdims=True)

    arrive(id_z)
    for zz in range(8):
        nid[40 * zz : 40 * zz + 40, :] = jnp.broadcast_to(column(idz[zz, 1:2, :], eye40), (40, 128))
    wanted = nid[...].reshape(8, 40, 128)
    for n in range(4):
        have = (z * 512 + n * 128 + 1 + iota((1, 128), 1)).astype(F32)
        selq[:, n * 128 : (n + 1) * 128] = onehot(wanted[:, 0:16].reshape(128, 128) == have)
        selk[:, n * 128 : (n + 1) * 128] = onehot(wanted[:, 16:40].reshape(192, 128) == have)

    arrive(x_plane)
    pair = halves(xpl[...].reshape(512, 128))
    sx[:, 0:16] = pick(selq[...], pair).reshape(8, 16, 128)

    def send_x(stage, first, count):
        return send_z(
            stage,
            lambda k: sx.at[lax.rem(z + k, 8), pl.ds(first, count)],
            xr.at[z, pl.ds(first, count)],
            xr.at[pl.ds(0, 7), pl.ds(first, count)],
        )

    x_hess = send_x(1, 0, 16)
    sx[:, 16:40] = pick(selk[...], pair).reshape(8, 24, 128)
    xr[z] = sx[z]
    c_plane = [send_p(2 + a, lambda k: cpl.at[a, p], cpl.at[a, p], cpl.at[a, pl.ds(0, 7)]) for a in range(2)]
    rows_all = send_g(2, lambda k: rows.at[g], rows.at[g], rows.at[pl.ds(0, 3)])

    eye = iota((128, 128), 0) == iota((128, 128), 1)

    def forward(first, pairs, source, store):
        def body(i, _):
            x8 = source(i)
            out = jnp.zeros((8, 128), F32)
            for h in range(2):
                for r in range(4):
                    total = None
                    for n in range(4):
                        part = tiles[first + 2 * i + h, r * 128 : (r + 1) * 128, n * 128 : (n + 1) * 128]
                        part = part * x8[4 * h + n : 4 * h + n + 1, :]
                        total = part if total is None else total + part
                    col = jnp.sum(total, axis=1, keepdims=True)
                    row = jnp.sum(jnp.where(eye, col, 0.0), axis=0, keepdims=True)
                    out = jnp.where(sub8 == 4 * h + r, row, out)
            store(i, out)
            return 0

        lax.fori_loop(0, pairs, body, 0, unroll=True)

    def transposed(stage):
        def body(i, _):
            y8 = yrows[pl.ds(pl.multiple_of(8 * i, 8), 8), :]
            out = jnp.zeros((8, 128), F32)
            for h in range(2):
                totals = [None] * 4
                for r in range(4):
                    col = column(y8[4 * h + r : 4 * h + r + 1, :], eye)
                    for n in range(4):
                        part = tiles[4 + 2 * i + h, r * 128 : (r + 1) * 128, n * 128 : (n + 1) * 128]
                        part = folded(part * col)
                        totals[n] = part if totals[n] is None else totals[n] + part
                for n in range(4):
                    row = jnp.sum(totals[n], axis=0, keepdims=True)
                    out = jnp.where(sub8 == 4 * h + n, row, out)
            zprod[stage, z, pl.ds(pl.multiple_of(16 + 8 * i, 8), 8), :] = -out
            return 0

        lax.fori_loop(0, 3, body, 0, unroll=True)

    def hess(step):
        def source(i):
            return xs[step, pl.ds(pl.multiple_of(64 + 8 * i, 8), 8), :]

        def store(i, out):
            zprod[step, z, pl.ds(pl.multiple_of(8 * i, 8), 8), :] = out

        forward(0, 2, source, store)

    def cons(step):
        def source(i):
            return xs[step, pl.ds(pl.multiple_of(80 + 8 * i, 8), 8), :]

        def store(i, out):
            kp[step, pl.ds(pl.multiple_of(8 * i, 8), 8), :] = out

        forward(4, 3, source, store)

    def send_products(stage, step, first, count):
        part = zprod.at[step, z, pl.ds(first, count)]
        return send_z(stage, lambda k: part, part, zprod.at[step, pl.ds(0, 7), pl.ds(first, count)])

    def picked(a):
        arrive(c_plane[a])
        pair = halves(cpl[a].reshape(512, 128))
        sc[a, :, 0:16] = pick(selq[...], pair).reshape(8, 16, 128)
        sc[a, :, 16:40] = pick(selk[...], pair).reshape(8, 24, 128)
        cr[a, z] = sc[a, z]
        cst[a, 0:64, :] = cpl[a, p]

    def send_constants(stage, a, n, first, count):
        return send_z(
            stage,
            lambda k: sc.at[pl.ds(a, n), lax.rem(z + k, 8), pl.ds(first, count)],
            cr.at[pl.ds(a, n), z, pl.ds(first, count)],
            cr.at[pl.ds(a, n), pl.ds(0, 7), pl.ds(first, count)],
        )

    arrive(id_g)
    eye32 = (iota((32, 128), 1) == iota((32, 128), 0) + g * 24) & (iota((32, 128), 0) < 24)
    ysel[...] = onehot(column(idg[g, 2:3, :], eye32) == (iota((32, 128), 1) + 1).astype(F32))
    arrive(y_all)
    ys[0] = y0[...].reshape(128, 128)
    loaded(7, tiles.at[pl.ds(0, 6)])
    yrows[...] = pick(ysel[...], halves(ys[0]))
    transposed(0)
    products = [send_products(10, 0, 16, 24)]
    x_cons = send_x(11, 16, 24)

    arrive(id_p)
    for pp in range(8):
        nidp[40 * pp : 40 * pp + 40, :] = jnp.broadcast_to(column(idp[pp, 1:2, :], eye40), (40, 128))
    for n in range(4):
        at = n * 128 + iota((1, 128), 1)
        have = (((at // 64) * 8 + p) * 64 + at % 64 + 1).astype(F32)
        selp[:, n * 128 : (n + 1) * 128] = onehot(nidp[...] == have)
    arrive(hi_line)
    sh[...] = pick(selp[...], halves(hz[...].reshape(512, 128))).reshape(8, 40, 128)
    hr[p] = sh[p]
    hi_slots = send_p(9, lambda k: sh.at[p_index(k)], hr.at[p], hr.at[pl.ds(0, 7)])

    loaded(8, tiles.at[pl.ds(0, 4)])
    arrive(x_hess)
    xs[0, 64:80, :] = jnp.sum(xr[:, 0:16, :], axis=0)
    hess(0)
    products.append(send_products(5, 0, 0, 16))

    picked(0)
    picked(1)

    own = (z * 512 + 1 + iota((512, 128), 0)).astype(F32)
    slots = nidp[...].reshape(8, 40, 128)
    for n in range(4):
        made = idz[2 * n, 0:1, :] + idz[2 * n + 1, 0:1, :]
        esk[:, n * 128 : (n + 1) * 128] = onehot(slots[:, 16:40].reshape(192, 128) == made)
        esq[:, n * 128 : (n + 1) * 128] = onehot(slots[:, 0:16].reshape(128, 128) == made)
        eo[:, n * 128 : (n + 1) * 128] = onehot(own == made)
    all_rows = idg[0, 2:3, :] + idg[1, 2:3, :] + idg[2, 2:3, :] + idg[3, 2:3, :]
    ed[...] = onehot((iota((128, 128), 0) + 1).astype(F32) == all_rows)[:, 0:96]


    def next_weight(sums, weight):
        total = jnp.sum(sums, axis=1, keepdims=True) + EPSILON
        return jnp.sqrt(weight * jnp.sqrt(total[1:2] / total[0:1]))

    def sum_over_plane(step, w_z):
        arrive(w_z)
        wp[step, p] = jnp.sum(wz[step], axis=0)
        return send_p((4, 11)[step], lambda k: wp.at[step, p], wp.at[step, p], wp.at[step, pl.ds(0, 7)])

    weight = jnp.ones((1, 1), F32)
    for step in range(2):
        arrive(products[0])
        if step == 0:
            cons_all = send_constants(2, 0, 2, 16, 24)
        arrive(products[1])
        pair = halves(zprod[step].reshape(512, 128))
        spk[step] = pick(esk[...], pair).reshape(8, 24, 128)
        gpk[step, p] = spk[step, p]
        grad_s = send_p(
            5 + 2 * step, lambda k: spk.at[step, p_index(k)], gpk.at[step, p], gpk.at[step, pl.ds(0, 7)]
        )

        def send_own():
            return send_p(6 + 2 * step, lambda k: spo.at[step, p_index(k)], gpo.at[step, p], gpo.at[step, pl.ds(0, 7)], OWN_ORDER)

        if step == 1:
            w_p = sum_over_plane(0, w_z)
        spo[step] = pick(eo[...], pair).reshape(8, 64, 128)
        gpo[step, p] = spo[step, p]
        if step == 0:
            arrive(x_cons)
            xs[0, 80:104, :] = jnp.sum(xr[:, 16:40, :], axis=0)
            cons(0)
            spq[...] = pick(esq[...], pair).reshape(8, 16, 128)
            gpq[p] = spq[p]
            grad_h = send_p(10, lambda k: spq.at[p_index(k)], gpq.at[p], gpq.at[pl.ds(0, 7)])
            grad_o = send_own()
            hess_all = send_constants(3, 0, 2, 0, 16)
            arrive(hi_slots)
            cst[2, 64:104, :] = jnp.sum(hr[...], axis=0)
            arrive(cons_all)
            for a in range(2):
                cst[a, 80:104, :] = jnp.sum(cr[a, :, 16:40, :], axis=0)
        if step == 1:
            grad_o = send_own()
        if step == 1:
            arrive(w_p)
            weight = next_weight(jnp.sum(wp[0], axis=0), weight)
        step_primal = STEP_SCALE / weight
        step_dual = STEP_SCALE * weight

        def advance(a, b, total):
            here = pl.ds(a, b - a)
            current = xs[step, here, :]
            moved = current - step_primal * (total + cst[0, here, :])
            updated = jnp.minimum(jnp.maximum(moved, cst[1, here, :]), cst[2, here, :])
            xs[step + 1, here, :] = updated
            return updated - current

        arrive(grad_s)
        advance(80, 104, jnp.sum(gpk[step], axis=0))

        cons(step + 1)
        dbuf[step, g] = 2.0 * kp[step + 1] - kp[step]
        duals_g = send_g(3 + step, lambda k: dbuf.at[step, g], dbuf.at[step, g], dbuf.at[step, pl.ds(0, 3)])
        arrive(grad_o)
        moved = advance(0, 64, jnp.sum(gpo[step], axis=0))
        wg[step, g] = jnp.sum(moved * moved, axis=0, keepdims=True)
        w_g = send_g(5 + step, lambda k: wg.at[step, g], wg.at[step, g], wg.at[step, pl.ds(0, 3)])
        if step == 1:
            xo[...] = xs[2, 0:64, :]
        if step == 0:
            arrive(hess_all)
            arrive(grad_h)
            for a in range(2):
                cst[a, 64:80, :] = jnp.sum(cr[a, :, 0:16, :], axis=0)
            advance(64, 80, jnp.sum(gpq[...], axis=0))
            hess(1)
            products = [send_products(6, 1, 0, 16)]
            arrive(rows_all)
        arrive(duals_g)
        extrap = pick(ed[...], halves(dbuf[step].reshape(96, 128)))
        duals = ys[step]
        dual_new = duals + step_dual * (rows[:, 0].reshape(128, 128) - extrap)
        dual_new = jnp.where(rows[:, 1].reshape(128, 128) == 1.0, jnp.maximum(dual_new, 0.0), dual_new)
        ys[step + 1] = dual_new
        if step == 0:
            yrows[...] = pick(ysel[...], halves(dual_new))
            transposed(1)
            products.append(send_products(7, 1, 16, 24))
        else:
            yo[...] = ys[2, pl.ds(pl.multiple_of(g * 32, 32), 32), :]
        moved = dual_new - duals
        wz[step, z, 1:2, :] = jnp.sum(moved * moved, axis=0, keepdims=True)
        arrive(w_g)
        wz[step, z, 0:1, :] = jnp.sum(wg[step], axis=0)
        w_z = send_z(8 + step, lambda k: wz.at[step, z], wz.at[step, z], wz.at[step, pl.ds(0, 7)])
        if step == 1:
            w_p = sum_over_plane(1, w_z)

    arrive(w_p)
    w_s[0, 0] = next_weight(jnp.sum(wp[1], axis=0), weight)[0, 0]
    for axis in range(3):
        arrive((lines.at[pl.ds(0, sent[axis] // 1024)], ssems.at[axis]))


def shards(primal, dual, objective, lower, upper, bound_kind, rhs, row_kind, q_tiles, q_index, k_tiles, k_rows, k_cols):
    hbm = pl.BlockSpec(memory_space=pl.ANY)
    smem = pl.BlockSpec(memory_space=pltpu.SMEM)
    vmem, dma = pltpu.VMEM, pltpu.SemaphoreType.DMA

    def lines(v):
        return v.reshape(-1, 128)

    final_x, final_y, weight = pl.pallas_call(
        kernel,
        name="pdhg",
        out_shape=(
            vmem((64, 128), F32),
            vmem((32, 128), F32),
            jax.ShapeDtypeStruct((1, 1), F32),
        ),
        in_specs=[hbm] * 13,
        out_specs=(pl.BlockSpec(memory_space=vmem), pl.BlockSpec(memory_space=vmem), smem),
        scratch_shapes=[
            vmem((10, 512, 512), F32),
            vmem((2, 64, 128), F32),
            vmem((64, 128), jnp.int32),
            vmem((32, 128), jnp.int32),
            vmem((8, 64, 128), F32),
            vmem((8, 40, 128), F32),
            vmem((8, 40, 128), F32),
            vmem((320, 128), F32),
            vmem((320, 512), BF16),
            vmem((8, 64, 128), F32),
            vmem((2, 8, 64, 128), F32),
            vmem((4, 32, 128), F32),
            vmem((4, 2, 32, 128), F32),
            vmem((8, 4, 128), F32),
            vmem((8, 4, 128), F32),
            vmem((4, 4, 128), F32),
            vmem((320, 128), F32),
            vmem((128, 512), BF16),
            vmem((192, 512), BF16),
            vmem((192, 512), BF16),
            vmem((128, 512), BF16),
            vmem((512, 512), BF16),
            vmem((128, 96), BF16),
            vmem((32, 128), BF16),
            vmem((8, 40, 128), F32),
            vmem((8, 40, 128), F32),
            vmem((2, 8, 40, 128), F32),
            vmem((2, 8, 40, 128), F32),
            vmem((3, 104, 128), F32),
            vmem((3, 104, 128), F32),
            vmem((32, 128), F32),
            vmem((3, 128, 128), F32),
            vmem((3, 24, 128), F32),
            vmem((2, 8, 64, 128), F32),
            vmem((2, 8, 24, 128), F32),
            vmem((8, 16, 128), F32),
            vmem((2, 8, 64, 128), F32),
            vmem((2, 8, 24, 128), F32),
            vmem((8, 16, 128), F32),
            vmem((2, 8, 64, 128), F32),
            vmem((2, 4, 24, 128), F32),
            vmem((2, 8, 2, 128), F32),
            vmem((2, 8, 2, 128), F32),
            vmem((2, 4, 1, 128), F32),
            pltpu.SMEM((1, 2, 4), jnp.int32),
            pltpu.SMEM((1, 6), jnp.int32),
            pltpu.SMEM((1, 6), jnp.int32),
            vmem((1600, 2, 128), F32),
            dma((9,)),
            dma((3,)),
            dma((16,)),
            dma((12,)),
            dma((7,)),
        ],
        compiler_params=pltpu.CompilerParams(
            collective_id=0, has_side_effects=True, vmem_limit_bytes=67043328 - 128 * 1024
        ),
    )(
        lines(primal), lines(dual), lines(objective), lines(lower), lines(upper), lines(bound_kind),
        lines(rhs), lines(row_kind), q_tiles, k_tiles, q_index, k_rows, k_cols,
    )
    return final_x.reshape(-1), final_y.reshape(-1), weight.reshape(())


def solution(mesh):
    finer = Mesh(mesh.devices.reshape(2, 2, 8, 4, 2), ("yh", "co", "z", "x", "yl"))
    grp, blk, both = ("yh", "co"), ("z", "x", "yl"), ("z", "x", "yl", "yh", "co")
    placed = (P(both),) * 8 + (
        P(grp, blk, None, None),
        P(grp, None, blk),
        P(grp, blk, None, None),
        P(grp, blk),
        P(grp, blk),
    )
    return jax.shard_map(shards, mesh=finer, in_specs=placed, out_specs=(P(both), P(both), P()), check_vma=False)
```

```python
import math

import jax
import jax.numpy as jnp
from jax import lax
from jax.experimental import pallas as pl
from jax.experimental.pallas import tpu as pltpu
from jax.sharding import Mesh
from jax.sharding import PartitionSpec as P

F32 = jnp.float32
BF16 = jnp.bfloat16
MESH = pl.DeviceIdType.MESH
EPSILON = 1e-06
STEP_SCALE = 0.5
FAR = 1e30
Z_ORDER = (4, 3, 5, 2, 6, 1, 7)
P_ORDER = (5, 4, 3, 7, 2, 6, 1)
OWN_ORDER = (5, 3, 7, 1, 4, 2, 6)
G_ORDER = (3, 2, 1)


def halves(v):
    hi = v.astype(BF16)
    mid = (v - hi.astype(F32)).astype(BF16)
    return jnp.concatenate([hi, mid], axis=1)


def pick(onehot, pair):
    both = jnp.dot(onehot, pair, preferred_element_type=F32)
    return both[:, 0:128] + both[:, 128:256]


def onehot(cond):
    return jnp.where(cond, 1.0, 0.0).astype(BF16)


def iota(shape, dim):
    return lax.broadcasted_iota(jnp.int32, shape, dim)


def folded(v):
    return jnp.sum(v.reshape(-1, 8, 128), axis=0)


def scalar_sum(v):
    return jnp.sum(jnp.sum(v, axis=0, keepdims=True), axis=1, keepdims=True)


def kernel(
    x_h, y_h, c_h, lo_h, hi_h, bk_h, b_h, rk_h, q_h, k_h, qi_h, kr_h, kc_h,
    xo, yo, w_s,
    tiles, bounds, kinds, rkind, hz, sh, hr, nidp, selp,
    xpl, cpl, y0, rows, idz, idp, idg, nid, selq, selk, esk, esq, eo, ed, ysel,
    sx, xr, sc, cr, xs, cst, yrows, ys, kp, zprod, spk, spq, spo, gpk, gpq, gpo, dbuf, wz, wp, wg,
    qi_s, kr_s, kc_s, lines, loc, ssems, zr, pr, gr,
):
    z = lax.axis_index("z")
    px, py = lax.axis_index("x"), lax.axis_index("yl")
    gh, gl = lax.axis_index("yh"), lax.axis_index("co")
    p, g = px * 2 + py, gh * 2 + gl
    sent = [0, 0, 0]

    def z_peer(k):
        return {"z": lax.rem(z + k, 8)}

    def p_peer(k):
        return {"x": lax.rem(px + k // 2, 4), "yl": lax.rem(py + k % 2, 2)}

    def g_peer(k):
        return {"yh": lax.rem(gh + k // 2, 2), "co": lax.rem(gl + k % 2, 2)}

    def p_index(k):
        return lax.rem(px + k // 2, 4) * 2 + lax.rem(py + k % 2, 2)

    barrier = pltpu.get_barrier_semaphore()
    for k in Z_ORDER:
        pl.semaphore_signal(barrier, inc=1, device_id=z_peer(k), device_id_type=MESH)
    for k in P_ORDER:
        pl.semaphore_signal(barrier, inc=1, device_id=p_peer(k), device_id_type=MESH)
    for k in G_ORDER:
        pl.semaphore_signal(barrier, inc=1, device_id=g_peer(k), device_id_type=MESH)

    def load(n, *pairs):
        for src, dst in pairs:
            pltpu.make_async_copy(src, dst, loc.at[n]).start()

    def loaded(n, part):
        pltpu.make_async_copy(part, part, loc.at[n]).wait()

    index_loads = [
        pltpu.make_async_copy(src, dst, loc.at[n])
        for n, (src, dst) in enumerate(((qi_h, qi_s), (kr_h, kr_s), (kc_h, kc_s)))
    ]
    for copy in index_loads:
        copy.start()
    load(3, (x_h, xpl.at[p]))
    load(4, (y_h, y0.at[g]))
    load(5, (c_h, cpl.at[0, p]), (lo_h, bounds.at[0]), (hi_h, bounds.at[1]), (bk_h, kinds))
    load(6, (b_h, rows.at[g, 0]), (rk_h, rkind))
    load(7, *((k_h.at[0, t], tiles.at[4 + t]) for t in range(6)))
    load(8, *((q_h.at[0, t], tiles.at[t]) for t in range(4)))

    def send(axis, order, peer, rsem, stage, source, target, whole):
        ssem = ssems.at[axis]
        for k in order:
            pltpu.make_async_remote_copy(
                src_ref=source(k), dst_ref=target, send_sem=ssem, recv_sem=rsem.at[stage],
                device_id=peer(k), device_id_type=MESH,
            ).start()
        sent[axis] += 4 * math.prod(whole.shape)
        return whole, rsem.at[stage]

    def send_z(stage, source, target, whole):
        return send(0, Z_ORDER, z_peer, zr, stage, source, target, whole)

    def send_p(stage, source, target, whole, order=P_ORDER):
        return send(1, order, p_peer, pr, stage, source, target, whole)

    def send_g(stage, source, target, whole):
        return send(2, G_ORDER, g_peer, gr, stage, source, target, whole)

    def arrive(stage):
        whole, sem = stage
        pltpu.make_async_copy(whole, whole, sem).wait()

    lane, sub = iota((4, 128), 1), iota((4, 128), 0)
    sub8 = iota((8, 128), 0)

    def ids_at(place, ids):
        slot = place // 4
        value = jnp.zeros((4, 128), jnp.int32)
        for n, scalar in enumerate(ids):
            value = jnp.where(slot == n, scalar, value)
        return jnp.where((place >= 0) & (place < 4 * len(ids)), value * 4 + place % 4 + 1, 0)

    for copy in index_loads:
        copy.wait()
    cons_cols = [kc_s[0, t] for t in range(6)]
    sent_v = ids_at(lane - lax.rem(z, 2) * 64, [qi_s[0, 0, t] for t in range(4)] + cons_cols)
    need_v = ids_at(lane, [qi_s[0, 1, t] for t in range(4)] + cons_cols)
    rows_v = ids_at(lane - g * 24, [kr_s[0, t] for t in range(6)])
    ids = jnp.where(sub == 0, sent_v, jnp.where(sub == 1, need_v, jnp.where(sub == 2, rows_v, 0))).astype(F32)
    idz[z] = ids
    idp[p] = ids
    idg[g] = ids
    for zz in range(8):
        zprod[0, zz, 40:64, :] = jnp.zeros((24, 128), F32)
        zprod[1, zz, 40:64, :] = jnp.zeros((24, 128), F32)

    pl.semaphore_wait(barrier, 17)

    id_z = send_z(0, lambda k: idz.at[z], idz.at[z], idz.at[pl.ds(0, 7)])
    loaded(3, x_h)
    x_plane = send_p(0, lambda k: xpl.at[p], xpl.at[p], xpl.at[pl.ds(0, 7)])
    id_g = send_g(0, lambda k: idg.at[g], idg.at[g], idg.at[pl.ds(0, 3)])
    id_p = send_p(1, lambda k: idp.at[p], idp.at[p], idp.at[pl.ds(0, 7)])
    loaded(4, y_h)
    y_all = send_g(1, lambda k: y0.at[g], y0.at[g], y0.at[pl.ds(0, 3)])
    loaded(5, cpl.at[0, pl.ds(0, 4)])
    kind = kinds[...]
    cpl[1, p] = jnp.where((kind == 1) | (kind == 2), bounds[0], -FAR)
    upper = jnp.where((kind == 2) | (kind == 3), bounds[1], FAR)
    hz[z] = upper
    hi_line = send_z(4, lambda k: hz.at[z], hz.at[z], hz.at[pl.ds(0, 7)])
    cst[2, 0:64, :] = upper
    loaded(6, rows.at[0])
    rows[g, 1] = rkind[...].astype(F32)
    xs[0, 0:64, :] = xpl[p]

    eye40 = iota((40, 128), 0) == iota((40, 128), 1)

    def column(row, mask):
        return jnp.sum(jnp.where(mask, row, 0.0), axis=1, keepdims=True)

    arrive(id_z)
    for zz in range(8):
        nid[40 * zz : 40 * zz + 40, :] = jnp.broadcast_to(column(idz[zz, 1:2, :], eye40), (40, 128))
    wanted = nid[...].reshape(8, 40, 128)
    for n in range(4):
        have = (z * 512 + n * 128 + 1 + iota((1, 128), 1)).astype(F32)
        selq[:, n * 128 : (n + 1) * 128] = onehot(wanted[:, 0:16].reshape(128, 128) == have)
        selk[:, n * 128 : (n + 1) * 128] = onehot(wanted[:, 16:40].reshape(192, 128) == have)

    arrive(x_plane)
    pair = halves(xpl[...].reshape(512, 128))
    sx[:, 0:16] = pick(selq[...], pair).reshape(8, 16, 128)

    def send_x(stage, first, count):
        return send_z(
            stage,
            lambda k: sx.at[lax.rem(z + k, 8), pl.ds(first, count)],
            xr.at[z, pl.ds(first, count)],
            xr.at[pl.ds(0, 7), pl.ds(first, count)],
        )

    x_hess = send_x(1, 0, 16)
    sx[:, 16:40] = pick(selk[...], pair).reshape(8, 24, 128)
    xr[z] = sx[z]
    c_plane = [send_p(2 + a, lambda k: cpl.at[a, p], cpl.at[a, p], cpl.at[a, pl.ds(0, 7)]) for a in range(2)]
    rows_all = send_g(2, lambda k: rows.at[g], rows.at[g], rows.at[pl.ds(0, 3)])

    eye = iota((128, 128), 0) == iota((128, 128), 1)

    def forward(first, pairs, source, store):
        def body(i, _):
            x8 = source(i)
            out = jnp.zeros((8, 128), F32)
            for h in range(2):
                for r in range(4):
                    total = None
                    for n in range(4):
                        part = tiles[first + 2 * i + h, r * 128 : (r + 1) * 128, n * 128 : (n + 1) * 128]
                        part = part * x8[4 * h + n : 4 * h + n + 1, :]
                        total = part if total is None else total + part
                    col = jnp.sum(total, axis=1, keepdims=True)
                    row = jnp.sum(jnp.where(eye, col, 0.0), axis=0, keepdims=True)
                    out = jnp.where(sub8 == 4 * h + r, row, out)
            store(i, out)
            return 0

        lax.fori_loop(0, pairs, body, 0, unroll=True)

    def transposed(stage):
        def body(i, _):
            y8 = yrows[pl.ds(pl.multiple_of(8 * i, 8), 8), :]
            out = jnp.zeros((8, 128), F32)
            for h in range(2):
                totals = [None] * 4
                for r in range(4):
                    col = column(y8[4 * h + r : 4 * h + r + 1, :], eye)
                    for n in range(4):
                        part = tiles[4 + 2 * i + h, r * 128 : (r + 1) * 128, n * 128 : (n + 1) * 128]
                        part = folded(part * col)
                        totals[n] = part if totals[n] is None else totals[n] + part
                for n in range(4):
                    row = jnp.sum(totals[n], axis=0, keepdims=True)
                    out = jnp.where(sub8 == 4 * h + n, row, out)
            zprod[stage, z, pl.ds(pl.multiple_of(16 + 8 * i, 8), 8), :] = -out
            return 0

        lax.fori_loop(0, 3, body, 0, unroll=True)

    def hess(step):
        def source(i):
            return xs[step, pl.ds(pl.multiple_of(64 + 8 * i, 8), 8), :]

        def store(i, out):
            zprod[step, z, pl.ds(pl.multiple_of(8 * i, 8), 8), :] = out

        forward(0, 2, source, store)

    def cons(step):
        def source(i):
            return xs[step, pl.ds(pl.multiple_of(80 + 8 * i, 8), 8), :]

        def store(i, out):
            kp[step, pl.ds(pl.multiple_of(8 * i, 8), 8), :] = out

        forward(4, 3, source, store)

    def send_products(stage, step, first, count):
        part = zprod.at[step, z, pl.ds(first, count)]
        return send_z(stage, lambda k: part, part, zprod.at[step, pl.ds(0, 7), pl.ds(first, count)])

    def picked(a):
        arrive(c_plane[a])
        pair = halves(cpl[a].reshape(512, 128))
        sc[a, :, 0:16] = pick(selq[...], pair).reshape(8, 16, 128)
        sc[a, :, 16:40] = pick(selk[...], pair).reshape(8, 24, 128)
        cr[a, z] = sc[a, z]
        cst[a, 0:64, :] = cpl[a, p]

    def send_constants(stage, a, n, first, count):
        return send_z(
            stage,
            lambda k: sc.at[pl.ds(a, n), lax.rem(z + k, 8), pl.ds(first, count)],
            cr.at[pl.ds(a, n), z, pl.ds(first, count)],
            cr.at[pl.ds(a, n), pl.ds(0, 7), pl.ds(first, count)],
        )

    arrive(id_g)
    eye32 = (iota((32, 128), 1) == iota((32, 128), 0) + g * 24) & (iota((32, 128), 0) < 24)
    ysel[...] = onehot(column(idg[g, 2:3, :], eye32) == (iota((32, 128), 1) + 1).astype(F32))
    arrive(y_all)
    ys[0] = y0[...].reshape(128, 128)
    loaded(7, tiles.at[pl.ds(0, 6)])
    yrows[...] = pick(ysel[...], halves(ys[0]))
    transposed(0)
    products = [send_products(10, 0, 16, 24)]
    x_cons = send_x(11, 16, 24)

    arrive(id_p)
    for pp in range(8):
        nidp[40 * pp : 40 * pp + 40, :] = jnp.broadcast_to(column(idp[pp, 1:2, :], eye40), (40, 128))
    for n in range(4):
        at = n * 128 + iota((1, 128), 1)
        have = (((at // 64) * 8 + p) * 64 + at % 64 + 1).astype(F32)
        selp[:, n * 128 : (n + 1) * 128] = onehot(nidp[...] == have)
    arrive(hi_line)
    sh[...] = pick(selp[...], halves(hz[...].reshape(512, 128))).reshape(8, 40, 128)
    hr[p] = sh[p]
    hi_slots = send_p(9, lambda k: sh.at[p_index(k)], hr.at[p], hr.at[pl.ds(0, 7)])

    loaded(8, tiles.at[pl.ds(0, 4)])
    arrive(x_hess)
    xs[0, 64:80, :] = jnp.sum(xr[:, 0:16, :], axis=0)
    hess(0)
    products.append(send_products(5, 0, 0, 16))

    picked(0)
    picked(1)

    own = (z * 512 + 1 + iota((512, 128), 0)).astype(F32)
    slots = nidp[...].reshape(8, 40, 128)
    for n in range(4):
        made = idz[2 * n, 0:1, :] + idz[2 * n + 1, 0:1, :]
        esk[:, n * 128 : (n + 1) * 128] = onehot(slots[:, 16:40].reshape(192, 128) == made)
        esq[:, n * 128 : (n + 1) * 128] = onehot(slots[:, 0:16].reshape(128, 128) == made)
        eo[:, n * 128 : (n + 1) * 128] = onehot(own == made)
    all_rows = idg[0, 2:3, :] + idg[1, 2:3, :] + idg[2, 2:3, :] + idg[3, 2:3, :]
    ed[...] = onehot((iota((128, 128), 0) + 1).astype(F32) == all_rows)[:, 0:96]


    def next_weight(sums, weight):
        total = jnp.sum(sums, axis=1, keepdims=True) + EPSILON
        return jnp.sqrt(weight * jnp.sqrt(total[1:2] / total[0:1]))

    def sum_over_plane(step, w_z):
        arrive(w_z)
        wp[step, p] = jnp.sum(wz[step], axis=0)
        return send_p((4, 11)[step], lambda k: wp.at[step, p], wp.at[step, p], wp.at[step, pl.ds(0, 7)])

    weight = jnp.ones((1, 1), F32)
    for step in range(2):
        arrive(products[0])
        if step == 0:
            cons_all = send_constants(2, 0, 2, 16, 24)
        arrive(products[1])
        pair = halves(zprod[step].reshape(512, 128))
        spk[step] = pick(esk[...], pair).reshape(8, 24, 128)
        gpk[step, p] = spk[step, p]
        grad_s = send_p(
            5 + 2 * step, lambda k: spk.at[step, p_index(k)], gpk.at[step, p], gpk.at[step, pl.ds(0, 7)]
        )

        def send_own():
            return send_p(6 + 2 * step, lambda k: spo.at[step, p_index(k)], gpo.at[step, p], gpo.at[step, pl.ds(0, 7)], OWN_ORDER)

        if step == 1:
            w_p = sum_over_plane(0, w_z)
        spo[step] = pick(eo[...], pair).reshape(8, 64, 128)
        gpo[step, p] = spo[step, p]
        if step == 0:
            arrive(x_cons)
            xs[0, 80:104, :] = jnp.sum(xr[:, 16:40, :], axis=0)
            cons(0)
            spq[...] = pick(esq[...], pair).reshape(8, 16, 128)
            gpq[p] = spq[p]
            grad_h = send_p(10, lambda k: spq.at[p_index(k)], gpq.at[p], gpq.at[pl.ds(0, 7)])
            grad_o = send_own()
            hess_all = send_constants(3, 0, 2, 0, 16)
            arrive(hi_slots)
            cst[2, 64:104, :] = jnp.sum(hr[...], axis=0)
            arrive(cons_all)
            for a in range(2):
                cst[a, 80:104, :] = jnp.sum(cr[a, :, 16:40, :], axis=0)
        if step == 1:
            grad_o = send_own()
        if step == 1:
            arrive(w_p)
            weight = next_weight(jnp.sum(wp[0], axis=0), weight)
        step_primal = STEP_SCALE / weight
        step_dual = STEP_SCALE * weight

        def advance(a, b, total):
            here = pl.ds(a, b - a)
            current = xs[step, here, :]
            moved = current - step_primal * (total + cst[0, here, :])
            updated = jnp.minimum(jnp.maximum(moved, cst[1, here, :]), cst[2, here, :])
            xs[step + 1, here, :] = updated
            return updated - current

        arrive(grad_s)
        advance(80, 104, jnp.sum(gpk[step], axis=0))

        cons(step + 1)
        dbuf[step, g] = 2.0 * kp[step + 1] - kp[step]
        duals_g = send_g(3 + step, lambda k: dbuf.at[step, g], dbuf.at[step, g], dbuf.at[step, pl.ds(0, 3)])
        arrive(grad_o)
        moved = advance(0, 64, jnp.sum(gpo[step], axis=0))
        wg[step, g] = jnp.sum(moved * moved, axis=0, keepdims=True)
        w_g = send_g(5 + step, lambda k: wg.at[step, g], wg.at[step, g], wg.at[step, pl.ds(0, 3)])
        if step == 1:
            xo[...] = xs[2, 0:64, :]
        if step == 0:
            arrive(hess_all)
            arrive(grad_h)
            for a in range(2):
                cst[a, 64:80, :] = jnp.sum(cr[a, :, 0:16, :], axis=0)
            advance(64, 80, jnp.sum(gpq[...], axis=0))
            hess(1)
            products = [send_products(6, 1, 0, 16)]
            arrive(rows_all)
        arrive(duals_g)
        extrap = pick(ed[...], halves(dbuf[step].reshape(96, 128)))
        duals = ys[step]
        dual_new = duals + step_dual * (rows[:, 0].reshape(128, 128) - extrap)
        dual_new = jnp.where(rows[:, 1].reshape(128, 128) == 1.0, jnp.maximum(dual_new, 0.0), dual_new)
        ys[step + 1] = dual_new
        if step == 0:
            yrows[...] = pick(ysel[...], halves(dual_new))
            transposed(1)
            products.append(send_products(7, 1, 16, 24))
        else:
            yo[...] = ys[2, pl.ds(pl.multiple_of(g * 32, 32), 32), :]
        moved = dual_new - duals
        wz[step, z, 1:2, :] = jnp.sum(moved * moved, axis=0, keepdims=True)
        arrive(w_g)
        wz[step, z, 0:1, :] = jnp.sum(wg[step], axis=0)
        w_z = send_z(8 + step, lambda k: wz.at[step, z], wz.at[step, z], wz.at[step, pl.ds(0, 7)])
        if step == 1:
            w_p = sum_over_plane(1, w_z)

    arrive(w_p)
    w_s[0, 0] = next_weight(jnp.sum(wp[1], axis=0), weight)[0, 0]
    for axis in range(3):
        arrive((lines.at[pl.ds(0, sent[axis] // 1024)], ssems.at[axis]))


def deliver(x, y, xo, yo, sem):
    copies = [pltpu.make_async_copy(x, xo, sem.at[0]), pltpu.make_async_copy(y, yo, sem.at[1])]
    for copy in copies:
        copy.start()
    for copy in copies:
        copy.wait()


def shards(primal, dual, objective, lower, upper, bound_kind, rhs, row_kind, q_tiles, q_index, k_tiles, k_rows, k_cols):
    hbm = pl.BlockSpec(memory_space=pl.ANY)
    smem = pl.BlockSpec(memory_space=pltpu.SMEM)
    vmem, dma = pltpu.VMEM, pltpu.SemaphoreType.DMA

    def lines(v):
        return v.reshape(-1, 128)

    final_x, final_y, weight = pl.pallas_call(
        kernel,
        name="pdhg",
        out_shape=(
            vmem((64, 128), F32),
            vmem((32, 128), F32),
            jax.ShapeDtypeStruct((1, 1), F32),
        ),
        in_specs=[hbm] * 13,
        out_specs=(pl.BlockSpec(memory_space=vmem), pl.BlockSpec(memory_space=vmem), smem),
        scratch_shapes=[
            vmem((10, 512, 512), F32),
            vmem((2, 64, 128), F32),
            vmem((64, 128), jnp.int32),
            vmem((32, 128), jnp.int32),
            vmem((8, 64, 128), F32),
            vmem((8, 40, 128), F32),
            vmem((8, 40, 128), F32),
            vmem((320, 128), F32),
            vmem((320, 512), BF16),
            vmem((8, 64, 128), F32),
            vmem((2, 8, 64, 128), F32),
            vmem((4, 32, 128), F32),
            vmem((4, 2, 32, 128), F32),
            vmem((8, 4, 128), F32),
            vmem((8, 4, 128), F32),
            vmem((4, 4, 128), F32),
            vmem((320, 128), F32),
            vmem((128, 512), BF16),
            vmem((192, 512), BF16),
            vmem((192, 512), BF16),
            vmem((128, 512), BF16),
            vmem((512, 512), BF16),
            vmem((128, 96), BF16),
            vmem((32, 128), BF16),
            vmem((8, 40, 128), F32),
            vmem((8, 40, 128), F32),
            vmem((2, 8, 40, 128), F32),
            vmem((2, 8, 40, 128), F32),
            vmem((3, 104, 128), F32),
            vmem((3, 104, 128), F32),
            vmem((32, 128), F32),
            vmem((3, 128, 128), F32),
            vmem((3, 24, 128), F32),
            vmem((2, 8, 64, 128), F32),
            vmem((2, 8, 24, 128), F32),
            vmem((8, 16, 128), F32),
            vmem((2, 8, 64, 128), F32),
            vmem((2, 8, 24, 128), F32),
            vmem((8, 16, 128), F32),
            vmem((2, 8, 64, 128), F32),
            vmem((2, 4, 24, 128), F32),
            vmem((2, 8, 2, 128), F32),
            vmem((2, 8, 2, 128), F32),
            vmem((2, 4, 1, 128), F32),
            pltpu.SMEM((1, 2, 4), jnp.int32),
            pltpu.SMEM((1, 6), jnp.int32),
            pltpu.SMEM((1, 6), jnp.int32),
            vmem((1600, 2, 128), F32),
            dma((9,)),
            dma((3,)),
            dma((16,)),
            dma((12,)),
            dma((7,)),
        ],
        compiler_params=pltpu.CompilerParams(
            collective_id=0, has_side_effects=True, vmem_limit_bytes=67043328 - 128 * 1024
        ),
    )(
        lines(primal), lines(dual), lines(objective), lines(lower), lines(upper), lines(bound_kind),
        lines(rhs), lines(row_kind), q_tiles, k_tiles, q_index, k_rows, k_cols,
    )
    final_x, final_y = pl.pallas_call(
        deliver,
        name="deliver",
        out_shape=(jax.ShapeDtypeStruct((64, 128), F32), jax.ShapeDtypeStruct((32, 128), F32)),
        in_specs=[pl.BlockSpec(memory_space=vmem)] * 2,
        out_specs=(hbm, hbm),
        scratch_shapes=[dma((2,))],
        compiler_params=pltpu.CompilerParams(vmem_limit_bytes=1024 * 1024),
    )(final_x, final_y)
    return final_x.reshape(-1), final_y.reshape(-1), weight.reshape(())


def solution(mesh):
    finer = Mesh(mesh.devices.reshape(2, 2, 8, 4, 2), ("yh", "co", "z", "x", "yl"))
    grp, blk, both = ("yh", "co"), ("z", "x", "yl"), ("z", "x", "yl", "yh", "co")
    placed = (P(both),) * 8 + (
        P(grp, blk, None, None),
        P(grp, None, blk),
        P(grp, blk, None, None),
        P(grp, blk),
        P(grp, blk),
    )
    return jax.shard_map(shards, mesh=finer, in_specs=placed, out_specs=(P(both), P(both), P()), check_vma=False)
```

```python
import math

import jax
import jax.numpy as jnp
from jax import lax
from jax.experimental import pallas as pl
from jax.experimental.pallas import tpu as pltpu
from jax.sharding import Mesh
from jax.sharding import PartitionSpec as P

F32 = jnp.float32
BF16 = jnp.bfloat16
MESH = pl.DeviceIdType.MESH
EPSILON = 1e-06
STEP_SCALE = 0.5
FAR = 1e30
Z_ORDER = (4, 3, 5, 2, 6, 1, 7)
P_ORDER = (5, 4, 3, 7, 2, 6, 1)
OWN_ORDER = (5, 3, 7, 1, 4, 2, 6)
G_ORDER = (3, 2, 1)


def halves(v):
    hi = v.astype(BF16)
    mid = (v - hi.astype(F32)).astype(BF16)
    return jnp.concatenate([hi, mid], axis=1)


def pick(onehot, pair):
    both = jnp.dot(onehot, pair, preferred_element_type=F32)
    return both[:, 0:128] + both[:, 128:256]


def onehot(cond):
    return jnp.where(cond, 1.0, 0.0).astype(BF16)


def iota(shape, dim):
    return lax.broadcasted_iota(jnp.int32, shape, dim)


def folded(v):
    return jnp.sum(v.reshape(-1, 8, 128), axis=0)


def scalar_sum(v):
    return jnp.sum(jnp.sum(v, axis=0, keepdims=True), axis=1, keepdims=True)


def kernel(
    x_h, y_h, c_h, lo_h, hi_h, bk_h, b_h, rk_h, q_h, k_h, qi_h, kr_h, kc_h,
    xo, yo, w_s,
    tiles, bounds, kinds, rkind, hz, sh, hr, nidp, selp,
    xpl, cpl, y0, rows, idz, idp, idg, nid, selq, selk, esk, esq, eo, ed, ysel,
    sx, xr, sc, cr, xs, cst, yrows, ys, kp, zprod, spk, spq, spo, gpk, gpq, gpo, dbuf, wz, wp, wg,
    qi_s, kr_s, kc_s, lines, loc, ssems, zr, pr, gr,
):
    z = lax.axis_index("z")
    px, py = lax.axis_index("x"), lax.axis_index("yl")
    gh, gl = lax.axis_index("yh"), lax.axis_index("co")
    p, g = px * 2 + py, gh * 2 + gl
    sent = [0, 0, 0]

    def z_peer(k):
        return {"z": lax.rem(z + k, 8)}

    def p_peer(k):
        return {"x": lax.rem(px + k // 2, 4), "yl": lax.rem(py + k % 2, 2)}

    def g_peer(k):
        return {"yh": lax.rem(gh + k // 2, 2), "co": lax.rem(gl + k % 2, 2)}

    def p_index(k):
        return lax.rem(px + k // 2, 4) * 2 + lax.rem(py + k % 2, 2)

    barrier = pltpu.get_barrier_semaphore()
    for k in Z_ORDER:
        pl.semaphore_signal(barrier, inc=1, device_id=z_peer(k), device_id_type=MESH)
    for k in P_ORDER:
        pl.semaphore_signal(barrier, inc=1, device_id=p_peer(k), device_id_type=MESH)
    for k in G_ORDER:
        pl.semaphore_signal(barrier, inc=1, device_id=g_peer(k), device_id_type=MESH)

    def load(n, *pairs):
        for src, dst in pairs:
            pltpu.make_async_copy(src, dst, loc.at[n]).start()

    def loaded(n, part):
        pltpu.make_async_copy(part, part, loc.at[n]).wait()

    index_loads = [
        pltpu.make_async_copy(src, dst, loc.at[n])
        for n, (src, dst) in enumerate(((qi_h, qi_s), (kr_h, kr_s), (kc_h, kc_s)))
    ]
    for copy in index_loads:
        copy.start()
    load(3, (x_h, xpl.at[p]))
    load(4, (y_h, y0.at[g]))
    load(5, (c_h, cpl.at[0, p]), (lo_h, bounds.at[0]), (hi_h, bounds.at[1]), (bk_h, kinds))
    load(6, (b_h, rows.at[g, 0]), (rk_h, rkind))
    load(7, *((k_h.at[0, t], tiles.at[4 + t]) for t in range(6)))
    load(8, *((q_h.at[0, t], tiles.at[t]) for t in range(4)))

    def send(axis, order, peer, rsem, stage, source, target, whole):
        ssem = ssems.at[axis]
        for k in order:
            pltpu.make_async_remote_copy(
                src_ref=source(k), dst_ref=target, send_sem=ssem, recv_sem=rsem.at[stage],
                device_id=peer(k), device_id_type=MESH,
            ).start()
        sent[axis] += 4 * math.prod(whole.shape)
        return whole, rsem.at[stage]

    def send_z(stage, source, target, whole):
        return send(0, Z_ORDER, z_peer, zr, stage, source, target, whole)

    def send_p(stage, source, target, whole, order=P_ORDER):
        return send(1, order, p_peer, pr, stage, source, target, whole)

    def send_g(stage, source, target, whole):
        return send(2, G_ORDER, g_peer, gr, stage, source, target, whole)

    def arrive(stage):
        whole, sem = stage
        pltpu.make_async_copy(whole, whole, sem).wait()

    lane, sub = iota((4, 128), 1), iota((4, 128), 0)
    sub8 = iota((8, 128), 0)

    def ids_at(place, ids):
        slot = place // 4
        value = jnp.zeros((4, 128), jnp.int32)
        for n, scalar in enumerate(ids):
            value = jnp.where(slot == n, scalar, value)
        return jnp.where((place >= 0) & (place < 4 * len(ids)), value * 4 + place % 4 + 1, 0)

    for copy in index_loads:
        copy.wait()
    cons_cols = [kc_s[0, t] for t in range(6)]
    sent_v = ids_at(lane - lax.rem(z, 2) * 64, [qi_s[0, 0, t] for t in range(4)] + cons_cols)
    need_v = ids_at(lane, [qi_s[0, 1, t] for t in range(4)] + cons_cols)
    rows_v = ids_at(lane - g * 24, [kr_s[0, t] for t in range(6)])
    ids = jnp.where(sub == 0, sent_v, jnp.where(sub == 1, need_v, jnp.where(sub == 2, rows_v, 0))).astype(F32)
    idz[z] = ids
    idp[p] = ids
    idg[g] = ids
    for zz in range(8):
        zprod[0, zz, 40:64, :] = jnp.zeros((24, 128), F32)
        zprod[1, zz, 40:64, :] = jnp.zeros((24, 128), F32)

    pl.semaphore_wait(barrier, 17)

    loaded(3, x_h)
    x_plane = send_p(0, lambda k: xpl.at[p], xpl.at[p], xpl.at[pl.ds(0, 7)])
    id_z = send_z(0, lambda k: idz.at[z], idz.at[z], idz.at[pl.ds(0, 7)])
    id_g = send_g(0, lambda k: idg.at[g], idg.at[g], idg.at[pl.ds(0, 3)])
    id_p = send_p(1, lambda k: idp.at[p], idp.at[p], idp.at[pl.ds(0, 7)])
    loaded(4, y_h)
    y_all = send_g(1, lambda k: y0.at[g], y0.at[g], y0.at[pl.ds(0, 3)])
    loaded(5, cpl.at[0, pl.ds(0, 4)])
    kind = kinds[...]
    cpl[1, p] = jnp.where((kind == 1) | (kind == 2), bounds[0], -FAR)
    upper = jnp.where((kind == 2) | (kind == 3), bounds[1], FAR)
    hz[z] = upper
    hi_line = send_z(4, lambda k: hz.at[z], hz.at[z], hz.at[pl.ds(0, 7)])
    cst[2, 0:64, :] = upper
    loaded(6, rows.at[0])
    rows[g, 1] = rkind[...].astype(F32)
    xs[0, 0:64, :] = xpl[p]

    eye40 = iota((40, 128), 0) == iota((40, 128), 1)

    def column(row, mask):
        return jnp.sum(jnp.where(mask, row, 0.0), axis=1, keepdims=True)

    arrive(id_z)
    for zz in range(8):
        nid[40 * zz : 40 * zz + 40, :] = jnp.broadcast_to(column(idz[zz, 1:2, :], eye40), (40, 128))
    wanted = nid[...].reshape(8, 40, 128)
    for n in range(4):
        have = (z * 512 + n * 128 + 1 + iota((1, 128), 1)).astype(F32)
        selq[:, n * 128 : (n + 1) * 128] = onehot(wanted[:, 0:16].reshape(128, 128) == have)
        selk[:, n * 128 : (n + 1) * 128] = onehot(wanted[:, 16:40].reshape(192, 128) == have)

    arrive(x_plane)
    pair = halves(xpl[...].reshape(512, 128))
    sx[:, 0:16] = pick(selq[...], pair).reshape(8, 16, 128)

    def send_x(stage, first, count):
        return send_z(
            stage,
            lambda k: sx.at[lax.rem(z + k, 8), pl.ds(first, count)],
            xr.at[z, pl.ds(first, count)],
            xr.at[pl.ds(0, 7), pl.ds(first, count)],
        )

    x_hess = send_x(1, 0, 16)
    sx[:, 16:40] = pick(selk[...], pair).reshape(8, 24, 128)
    xr[z] = sx[z]
    c_plane = [send_p(2 + a, lambda k: cpl.at[a, p], cpl.at[a, p], cpl.at[a, pl.ds(0, 7)]) for a in range(2)]
    rows_all = send_g(2, lambda k: rows.at[g], rows.at[g], rows.at[pl.ds(0, 3)])

    eye = iota((128, 128), 0) == iota((128, 128), 1)

    def forward(first, pairs, source, store):
        def body(i, _):
            x8 = source(i)
            out = jnp.zeros((8, 128), F32)
            for h in range(2):
                for r in range(4):
                    total = None
                    for n in range(4):
                        part = tiles[first + 2 * i + h, r * 128 : (r + 1) * 128, n * 128 : (n + 1) * 128]
                        part = part * x8[4 * h + n : 4 * h + n + 1, :]
                        total = part if total is None else total + part
                    col = jnp.sum(total, axis=1, keepdims=True)
                    row = jnp.sum(jnp.where(eye, col, 0.0), axis=0, keepdims=True)
                    out = jnp.where(sub8 == 4 * h + r, row, out)
            store(i, out)
            return 0

        lax.fori_loop(0, pairs, body, 0, unroll=True)

    def transposed(stage):
        def body(i, _):
            y8 = yrows[pl.ds(pl.multiple_of(8 * i, 8), 8), :]
            out = jnp.zeros((8, 128), F32)
            for h in range(2):
                totals = [None] * 4
                for r in range(4):
                    col = column(y8[4 * h + r : 4 * h + r + 1, :], eye)
                    for n in range(4):
                        part = tiles[4 + 2 * i + h, r * 128 : (r + 1) * 128, n * 128 : (n + 1) * 128]
                        part = folded(part * col)
                        totals[n] = part if totals[n] is None else totals[n] + part
                for n in range(4):
                    row = jnp.sum(totals[n], axis=0, keepdims=True)
                    out = jnp.where(sub8 == 4 * h + n, row, out)
            zprod[stage, z, pl.ds(pl.multiple_of(16 + 8 * i, 8), 8), :] = -out
            return 0

        lax.fori_loop(0, 3, body, 0, unroll=True)

    def hess(step):
        def source(i):
            return xs[step, pl.ds(pl.multiple_of(64 + 8 * i, 8), 8), :]

        def store(i, out):
            zprod[step, z, pl.ds(pl.multiple_of(8 * i, 8), 8), :] = out

        forward(0, 2, source, store)

    def cons(step):
        def source(i):
            return xs[step, pl.ds(pl.multiple_of(80 + 8 * i, 8), 8), :]

        def store(i, out):
            kp[step, pl.ds(pl.multiple_of(8 * i, 8), 8), :] = out

        forward(4, 3, source, store)

    def send_products(stage, step, first, count):
        part = zprod.at[step, z, pl.ds(first, count)]
        return send_z(stage, lambda k: part, part, zprod.at[step, pl.ds(0, 7), pl.ds(first, count)])

    def picked(a):
        arrive(c_plane[a])
        pair = halves(cpl[a].reshape(512, 128))
        sc[a, :, 0:16] = pick(selq[...], pair).reshape(8, 16, 128)
        sc[a, :, 16:40] = pick(selk[...], pair).reshape(8, 24, 128)
        cr[a, z] = sc[a, z]
        cst[a, 0:64, :] = cpl[a, p]

    def send_constants(stage, a, n, first, count):
        return send_z(
            stage,
            lambda k: sc.at[pl.ds(a, n), lax.rem(z + k, 8), pl.ds(first, count)],
            cr.at[pl.ds(a, n), z, pl.ds(first, count)],
            cr.at[pl.ds(a, n), pl.ds(0, 7), pl.ds(first, count)],
        )

    arrive(id_g)
    eye32 = (iota((32, 128), 1) == iota((32, 128), 0) + g * 24) & (iota((32, 128), 0) < 24)
    ysel[...] = onehot(column(idg[g, 2:3, :], eye32) == (iota((32, 128), 1) + 1).astype(F32))
    arrive(y_all)
    ys[0] = y0[...].reshape(128, 128)
    loaded(7, tiles.at[pl.ds(0, 6)])
    yrows[...] = pick(ysel[...], halves(ys[0]))
    transposed(0)
    products = [send_products(10, 0, 16, 24)]
    x_cons = send_x(11, 16, 24)

    arrive(id_p)
    for pp in range(8):
        nidp[40 * pp : 40 * pp + 40, :] = jnp.broadcast_to(column(idp[pp, 1:2, :], eye40), (40, 128))
    for n in range(4):
        at = n * 128 + iota((1, 128), 1)
        have = (((at // 64) * 8 + p) * 64 + at % 64 + 1).astype(F32)
        selp[:, n * 128 : (n + 1) * 128] = onehot(nidp[...] == have)
    arrive(hi_line)
    sh[...] = pick(selp[...], halves(hz[...].reshape(512, 128))).reshape(8, 40, 128)
    hr[p] = sh[p]
    hi_slots = send_p(9, lambda k: sh.at[p_index(k)], hr.at[p], hr.at[pl.ds(0, 7)])

    loaded(8, tiles.at[pl.ds(0, 4)])
    arrive(x_hess)
    xs[0, 64:80, :] = jnp.sum(xr[:, 0:16, :], axis=0)
    hess(0)
    products.append(send_products(5, 0, 0, 16))

    picked(0)
    picked(1)

    own = (z * 512 + 1 + iota((512, 128), 0)).astype(F32)
    slots = nidp[...].reshape(8, 40, 128)
    for n in range(4):
        made = idz[2 * n, 0:1, :] + idz[2 * n + 1, 0:1, :]
        esk[:, n * 128 : (n + 1) * 128] = onehot(slots[:, 16:40].reshape(192, 128) == made)
        esq[:, n * 128 : (n + 1) * 128] = onehot(slots[:, 0:16].reshape(128, 128) == made)
        eo[:, n * 128 : (n + 1) * 128] = onehot(own == made)
    all_rows = idg[0, 2:3, :] + idg[1, 2:3, :] + idg[2, 2:3, :] + idg[3, 2:3, :]
    ed[...] = onehot((iota((128, 128), 0) + 1).astype(F32) == all_rows)[:, 0:96]


    def next_weight(sums, weight):
        total = jnp.sum(sums, axis=1, keepdims=True) + EPSILON
        return jnp.sqrt(weight * jnp.sqrt(total[1:2] / total[0:1]))

    def sum_over_plane(step, w_z):
        arrive(w_z)
        wp[step, p] = jnp.sum(wz[step], axis=0)
        return send_p((4, 11)[step], lambda k: wp.at[step, p], wp.at[step, p], wp.at[step, pl.ds(0, 7)])

    weight = jnp.ones((1, 1), F32)
    for step in range(2):
        arrive(products[0])
        if step == 0:
            cons_all = send_constants(2, 0, 2, 16, 24)
        arrive(products[1])
        pair = halves(zprod[step].reshape(512, 128))
        spk[step] = pick(esk[...], pair).reshape(8, 24, 128)
        gpk[step, p] = spk[step, p]
        grad_s = send_p(
            5 + 2 * step, lambda k: spk.at[step, p_index(k)], gpk.at[step, p], gpk.at[step, pl.ds(0, 7)]
        )

        def send_own():
            return send_p(6 + 2 * step, lambda k: spo.at[step, p_index(k)], gpo.at[step, p], gpo.at[step, pl.ds(0, 7)], OWN_ORDER)

        if step == 1:
            w_p = sum_over_plane(0, w_z)
        spo[step] = pick(eo[...], pair).reshape(8, 64, 128)
        gpo[step, p] = spo[step, p]
        if step == 0:
            arrive(x_cons)
            xs[0, 80:104, :] = jnp.sum(xr[:, 16:40, :], axis=0)
            cons(0)
            spq[...] = pick(esq[...], pair).reshape(8, 16, 128)
            gpq[p] = spq[p]
            grad_h = send_p(10, lambda k: spq.at[p_index(k)], gpq.at[p], gpq.at[pl.ds(0, 7)])
            grad_o = send_own()
            hess_all = send_constants(3, 0, 2, 0, 16)
            arrive(hi_slots)
            cst[2, 64:104, :] = jnp.sum(hr[...], axis=0)
            arrive(cons_all)
            for a in range(2):
                cst[a, 80:104, :] = jnp.sum(cr[a, :, 16:40, :], axis=0)
        if step == 1:
            grad_o = send_own()
        if step == 1:
            arrive(w_p)
            weight = next_weight(jnp.sum(wp[0], axis=0), weight)
        step_primal = STEP_SCALE / weight
        step_dual = STEP_SCALE * weight

        def advance(a, b, total):
            here = pl.ds(a, b - a)
            current = xs[step, here, :]
            moved = current - step_primal * (total + cst[0, here, :])
            updated = jnp.minimum(jnp.maximum(moved, cst[1, here, :]), cst[2, here, :])
            xs[step + 1, here, :] = updated
            return updated - current

        arrive(grad_s)
        advance(80, 104, jnp.sum(gpk[step], axis=0))

        cons(step + 1)
        dbuf[step, g] = 2.0 * kp[step + 1] - kp[step]
        duals_g = send_g(3 + step, lambda k: dbuf.at[step, g], dbuf.at[step, g], dbuf.at[step, pl.ds(0, 3)])
        arrive(grad_o)
        moved = advance(0, 64, jnp.sum(gpo[step], axis=0))
        wg[step, g] = jnp.sum(moved * moved, axis=0, keepdims=True)
        w_g = send_g(5 + step, lambda k: wg.at[step, g], wg.at[step, g], wg.at[step, pl.ds(0, 3)])
        if step == 1:
            xo[...] = xs[2, 0:64, :]
        if step == 0:
            arrive(hess_all)
            arrive(grad_h)
            for a in range(2):
                cst[a, 64:80, :] = jnp.sum(cr[a, :, 0:16, :], axis=0)
            advance(64, 80, jnp.sum(gpq[...], axis=0))
            hess(1)
            products = [send_products(6, 1, 0, 16)]
            arrive(rows_all)
        arrive(duals_g)
        extrap = pick(ed[...], halves(dbuf[step].reshape(96, 128)))
        duals = ys[step]
        dual_new = duals + step_dual * (rows[:, 0].reshape(128, 128) - extrap)
        dual_new = jnp.where(rows[:, 1].reshape(128, 128) == 1.0, jnp.maximum(dual_new, 0.0), dual_new)
        ys[step + 1] = dual_new
        if step == 0:
            yrows[...] = pick(ysel[...], halves(dual_new))
            transposed(1)
            products.append(send_products(7, 1, 16, 24))
        else:
            yo[...] = ys[2, pl.ds(pl.multiple_of(g * 32, 32), 32), :]
        moved = dual_new - duals
        wz[step, z, 1:2, :] = jnp.sum(moved * moved, axis=0, keepdims=True)
        arrive(w_g)
        wz[step, z, 0:1, :] = jnp.sum(wg[step], axis=0)
        w_z = send_z(8 + step, lambda k: wz.at[step, z], wz.at[step, z], wz.at[step, pl.ds(0, 7)])
        if step == 1:
            w_p = sum_over_plane(1, w_z)

    arrive(w_p)
    w_s[0, 0] = next_weight(jnp.sum(wp[1], axis=0), weight)[0, 0]
    for axis in range(3):
        arrive((lines.at[pl.ds(0, sent[axis] // 1024)], ssems.at[axis]))


def deliver(x, y, xo, yo, sem):
    copies = [pltpu.make_async_copy(x, xo, sem.at[0]), pltpu.make_async_copy(y, yo, sem.at[1])]
    for copy in copies:
        copy.start()
    for copy in copies:
        copy.wait()


def shards(primal, dual, objective, lower, upper, bound_kind, rhs, row_kind, q_tiles, q_index, k_tiles, k_rows, k_cols):
    hbm = pl.BlockSpec(memory_space=pl.ANY)
    smem = pl.BlockSpec(memory_space=pltpu.SMEM)
    vmem, dma = pltpu.VMEM, pltpu.SemaphoreType.DMA

    def lines(v):
        return v.reshape(-1, 128)

    final_x, final_y, weight = pl.pallas_call(
        kernel,
        name="pdhg",
        out_shape=(
            vmem((64, 128), F32),
            vmem((32, 128), F32),
            jax.ShapeDtypeStruct((1, 1), F32),
        ),
        in_specs=[hbm] * 13,
        out_specs=(pl.BlockSpec(memory_space=vmem), pl.BlockSpec(memory_space=vmem), smem),
        scratch_shapes=[
            vmem((10, 512, 512), F32),
            vmem((2, 64, 128), F32),
            vmem((64, 128), jnp.int32),
            vmem((32, 128), jnp.int32),
            vmem((8, 64, 128), F32),
            vmem((8, 40, 128), F32),
            vmem((8, 40, 128), F32),
            vmem((320, 128), F32),
            vmem((320, 512), BF16),
            vmem((8, 64, 128), F32),
            vmem((2, 8, 64, 128), F32),
            vmem((4, 32, 128), F32),
            vmem((4, 2, 32, 128), F32),
            vmem((8, 4, 128), F32),
            vmem((8, 4, 128), F32),
            vmem((4, 4, 128), F32),
            vmem((320, 128), F32),
            vmem((128, 512), BF16),
            vmem((192, 512), BF16),
            vmem((192, 512), BF16),
            vmem((128, 512), BF16),
            vmem((512, 512), BF16),
            vmem((128, 96), BF16),
            vmem((32, 128), BF16),
            vmem((8, 40, 128), F32),
            vmem((8, 40, 128), F32),
            vmem((2, 8, 40, 128), F32),
            vmem((2, 8, 40, 128), F32),
            vmem((3, 104, 128), F32),
            vmem((3, 104, 128), F32),
            vmem((32, 128), F32),
            vmem((3, 128, 128), F32),
            vmem((3, 24, 128), F32),
            vmem((2, 8, 64, 128), F32),
            vmem((2, 8, 24, 128), F32),
            vmem((8, 16, 128), F32),
            vmem((2, 8, 64, 128), F32),
            vmem((2, 8, 24, 128), F32),
            vmem((8, 16, 128), F32),
            vmem((2, 8, 64, 128), F32),
            vmem((2, 4, 24, 128), F32),
            vmem((2, 8, 2, 128), F32),
            vmem((2, 8, 2, 128), F32),
            vmem((2, 4, 1, 128), F32),
            pltpu.SMEM((1, 2, 4), jnp.int32),
            pltpu.SMEM((1, 6), jnp.int32),
            pltpu.SMEM((1, 6), jnp.int32),
            vmem((1600, 2, 128), F32),
            dma((9,)),
            dma((3,)),
            dma((12,)),
            dma((12,)),
            dma((7,)),
        ],
        compiler_params=pltpu.CompilerParams(
            collective_id=0, has_side_effects=True, vmem_limit_bytes=67043328 - 128 * 1024
        ),
    )(
        lines(primal), lines(dual), lines(objective), lines(lower), lines(upper), lines(bound_kind),
        lines(rhs), lines(row_kind), q_tiles, k_tiles, q_index, k_rows, k_cols,
    )
    final_x, final_y = pl.pallas_call(
        deliver,
        name="deliver",
        out_shape=(jax.ShapeDtypeStruct((64, 128), F32), jax.ShapeDtypeStruct((32, 128), F32)),
        in_specs=[pl.BlockSpec(memory_space=vmem)] * 2,
        out_specs=(hbm, hbm),
        scratch_shapes=[dma((2,))],
        compiler_params=pltpu.CompilerParams(vmem_limit_bytes=1024 * 1024),
    )(final_x, final_y)
    return final_x.reshape(-1), final_y.reshape(-1), weight.reshape(())


def solution(mesh):
    finer = Mesh(mesh.devices.reshape(2, 2, 8, 4, 2), ("yh", "co", "z", "x", "yl"))
    grp, blk, both = ("yh", "co"), ("z", "x", "yl"), ("z", "x", "yl", "yh", "co")
    placed = (P(both),) * 8 + (
        P(grp, blk, None, None),
        P(grp, None, blk),
        P(grp, blk, None, None),
        P(grp, blk),
        P(grp, blk),
    )
    return jax.shard_map(shards, mesh=finer, in_specs=placed, out_specs=(P(both), P(both), P()), check_vma=False)
```
